32 devices in a mesh: slab: 8 (over z, x), rhs: 4 (over y, core).
Axes of the slice: x: 2, y: 2, z: 4, core: 2. Of those that a mesh axis runs over, the one named last changes fastest.
Arguments:
- targets: float32 [8, 128, 256], P('rhs', 'slab'), may hold values from -60 to 60
- counts: int32 [128], P('slab'), may hold values from 1 to 256, 20480 in all
- cell_rows: int32 [128, 256], P('slab'), may hold values from 0 to 255
- cell_cols: int32 [128, 256], P('slab'), may hold values from 0 to 127
- fractions: float32 [2, 128, 256], P(None, 'slab'), may hold values from 0 to 1
- spectrum: float32 [2048, 2048], P(None, ('slab', 'rhs')), may hold values from 0.25 to 4, as said below
- noise_var: float32 [1], replicated, may hold values from 0.1 to 1
Outputs:
- solution: float32 [8, 128, 256], P('rhs', 'slab')
- residual: float32 [8, 128, 256], P('rhs', 'slab')
The draws below stay inside these ranges and needn't reach their ends.
Inputs may be any that keep to these rules, and one draw needn't show every extreme that they name: Each tile has 256 slots; tile t holds points in its first counts[t] slots, and the other slots are empty: their entries are ignored and their outputs are zero. Even in frequency: spectrum[a, b] = spectrum[(2048 - a) % 2048, (2048 - b) % 2048].
All inputs are finite; a program needn't handle non-finite values. No bound on the sum of `counts` on one device may be relied on, other than what follows from the above.
Results may differ from the reference program's by a relative error of at most 0.0002.
Values sent between devices are 32-bit elements; how exact they have to be, the bound alone decides.
No kernel may reach another device: no remote copies, remote signals or barrier semaphores. Data moves between devices by JAX's collectives and lax.ppermute only.
A program may use at most 128 MiB of HBM per device.

```python
import math
import jax
import jax.numpy as jnp
import numpy as np
from jax import lax

G = 2048
TC = 128
CAP = 256
RHS = 8
ITERS = 2
ROWS_DEV = 256
TILES = 16
TILES_ALL = 128


def draw_targets(key, part):
    position = jnp.arange(TILES_ALL, dtype=jnp.float32) / TILES_ALL
    growth = jnp.exp(jnp.log(3.0) * position)[None, :, None]
    values = jax.random.normal(key, (RHS, TILES_ALL, CAP), jnp.float32) * growth
    return jnp.clip(values, -60.0, 60.0)


def draw_spectrum(key, part):
    values = jnp.exp(jax.random.uniform(key, (G, G), jnp.float32, math.log(0.25), math.log(4.0)))
    mirrored = jnp.roll(jnp.flip(values, (0, 1)), 1, (0, 1))
    return jnp.clip(0.5 * (values + mirrored), 0.25, 4.0)


def plant(array, stream_key, low, top_value):
    longest = array.shape.index(max(array.shape))
    spots = []
    for shift in (0, 1):
        where = [jax.random.randint(jax.random.fold_in(stream_key, axis), (), 0, length) for axis, length in enumerate(array.shape)]
        where[longest] = (where[longest] + shift) % array.shape[longest]
        spots.append(tuple(where))
    return array.at[spots[0]].set(low).at[spots[1]].set(top_value)


def levels(own_key, dims, pieces, low, top_value):
    loudness, own = 1.0, jax.random.fold_in(own_key, 6)
    for dim, blocks in pieces:
        steps = jnp.exp(jax.random.uniform(jax.random.fold_in(own, dim), (blocks,), jnp.float32, low / len(pieces), top_value / len(pieces)))
        loudness = loudness * jnp.repeat(steps, dims[dim] // blocks).reshape([-1 if axis == dim else 1 for axis in range(len(dims))])
    return loudness


def split_up(amount, total, bound, lean):
    portions = [(1 << 20) // math.isqrt(grade ** lean) + 1 for grade in range(2, amount + 1)]
    spare, given = total - bound - (amount - 1), [1] * (amount - 1)
    while spare > 0:
        free = [i for i in range(amount - 1) if given[i] < bound]
        mass, remaining = sum([portions[i] for i in free]), spare
        for i in free:
            more = min(bound - given[i], max(1, remaining * portions[i] // mass), spare)
            given[i] = given[i] + more
            spare = spare - more
    return np.array([bound] + given)


def uneven(stream_key, amount, total, most, slope):
    if amount == 2:
        one = jax.random.randint(stream_key, (), max(1, total - most), min(most, total - 1) + 1)
        return jnp.stack([one, total - one])
    sizes = jnp.asarray(split_up(amount, total, most, slope), jnp.int32)
    twos = (amount - 1) // 2
    giver, sink = sizes[1:1 + 2 * twos:2], sizes[2:2 + 2 * twos:2]
    slack = jnp.minimum(giver - 1, most - sink)
    moved = jax.random.randint(jax.random.fold_in(stream_key, 1), (twos,), 0, 1 << 20) % (slack + 1)
    sizes = sizes.at[1:1 + 2 * twos:2].set(giver - moved).at[2:2 + 2 * twos:2].set(sink + moved)
    return sizes[jax.random.permutation(jax.random.fold_in(stream_key, 2), amount)]


def setup_inputs(seed: int = 0) -> dict:
    splits = jax.random.split(jax.random.key(seed), 8)
    return {
        "targets": draw_targets(jax.random.fold_in(splits[7], 71), 0),
        "counts": uneven(splits[1], TILES_ALL, TILES_ALL * CAP * 5 // 8, CAP, 2).astype(jnp.int32),
        "cell_rows": plant(jax.random.randint(splits[2], (TILES_ALL, CAP), 0, ROWS_DEV), jax.random.fold_in(splits[2], 1), 0, ROWS_DEV - 1).astype(jnp.int32),
        "cell_cols": plant(jax.random.randint(splits[3], (TILES_ALL, CAP), 0, TC), jax.random.fold_in(splits[3], 1), 0, TC - 1).astype(jnp.int32),
        "fractions": jnp.clip(1.0 * jax.random.uniform(splits[4], (2, TILES_ALL, CAP), jnp.float32) ** levels(splits[4], (2, TILES_ALL, CAP), ((1, 8),), -0.2, 0.2), 0.0, 1.0),
        "spectrum": draw_spectrum(jax.random.fold_in(splits[7], 71), 0),
        "noise_var": jnp.clip(jnp.exp(jax.random.uniform(splits[6], (1,), jnp.float32, math.log(0.1), math.log(1.0))), 0.1, 1.0),
    }


def cubic_weights(fraction):
    return (((-0.5 * fraction + 1.0) * fraction - 0.5) * fraction,
            (1.5 * fraction - 2.5) * fraction * fraction + 1.0,
            ((-1.5 * fraction + 2.0) * fraction + 0.5) * fraction,
            (0.5 * fraction - 0.5) * fraction * fraction)


def stencil(counts, cell_rows, cell_cols, fractions):
    tile_ids = jnp.arange(TILES_ALL, dtype=jnp.int32)
    row_base = (tile_ids // TILES) * ROWS_DEV
    col_base = (tile_ids % TILES) * TC
    grid_rows = row_base[:, None] + cell_rows
    grid_cols = col_base[:, None] + cell_cols
    slot_ids = jnp.arange(CAP, dtype=jnp.int32)
    live = (slot_ids[None, :] < counts[:, None]).astype(jnp.float32)
    row_weights = cubic_weights(fractions[0])
    col_weights = cubic_weights(fractions[1])
    indices = []
    weights = []
    for row_shift in range(4):
        for col_shift in range(4):
            rows_at = (grid_rows - 1 + row_shift) % G
            cols_at = (grid_cols - 1 + col_shift) % G
            indices.append((rows_at * G + cols_at).astype(jnp.int32).reshape(-1))
            weights.append(row_weights[row_shift] * col_weights[col_shift])
    return live, indices, weights


def kernel_product(grid_field, spectrum):
    return jnp.real(jnp.fft.ifft2(spectrum * jnp.fft.fft2(grid_field))).astype(jnp.float32)


def apply_operator(vector, live, indices, weights, spectrum, noise_var):
    grid_flat = jnp.zeros((RHS, G * G), jnp.float32)
    for flat_index, weight in zip(indices, weights):
        grid_flat = grid_flat.at[:, flat_index].add((weight[None] * vector).reshape(RHS, -1))
    grid = grid_flat.reshape(RHS, G, G)
    smoothed = lax.map(lambda grid_field: kernel_product(grid_field, spectrum), grid)
    smooth_flat = smoothed.reshape(RHS, G * G)
    result = jnp.zeros(vector.shape, jnp.float32)
    for flat_index, weight in zip(indices, weights):
        picked = jnp.take(smooth_flat, flat_index, axis=1).reshape(vector.shape)
        result = result + weight[None] * picked
    return live[None] * result + noise_var[0] * vector


def reference(targets, counts, cell_rows, cell_cols, fractions, spectrum, noise_var):
    live, indices, weights = stencil(counts, cell_rows, cell_cols, fractions)
    residual = live[None] * targets
    direction = residual
    solution = jnp.zeros(residual.shape, jnp.float32)
    norm_now = jnp.sum(residual * residual, axis=(1, 2))
    for repeat in range(ITERS):
        image = apply_operator(direction, live, indices, weights, spectrum, noise_var)
        alpha = norm_now / jnp.sum(direction * image, axis=(1, 2))
        solution = solution + alpha[:, None, None] * direction
        residual = residual - alpha[:, None, None] * image
        if repeat + 1 < ITERS:
            norm_next = jnp.sum(residual * residual, axis=(1, 2))
            direction = residual + (norm_next / norm_now)[:, None, None] * direction
            norm_now = norm_next
    return solution, residual
```

```python
import math

import jax
import jax.numpy as jnp
import ml_dtypes
import numpy as np
from jax import lax
from jax.experimental import pallas as pl
from jax.experimental.pallas import tpu as pltpu
from jax.sharding import PartitionSpec as P

G = 2048
TC = 128
ITERS = 2
WIN = 2 * TC
GEOM_ROWS = 24
VMEM_BYTES = 60000 * 1024


def cubic_weights(fraction):
    return (
        ((-0.5 * fraction + 1.0) * fraction - 0.5) * fraction,
        (1.5 * fraction - 2.5) * fraction * fraction + 1.0,
        ((-1.5 * fraction + 2.0) * fraction + 0.5) * fraction,
        (0.5 * fraction - 0.5) * fraction * fraction,
    )


def halves_np(table):
    high = table.astype(np.float32).astype(ml_dtypes.bfloat16)
    low = (table - high.astype(np.float64)).astype(np.float32).astype(ml_dtypes.bfloat16)
    return high, low


def angle_tables(rows, cols, length):
    index = (np.arange(rows)[:, None] * np.arange(cols)[None, :]) % length
    angle = index * (2.0 * math.pi / length)
    return np.cos(angle), np.sin(angle)


def row_matrices(size):
    cos_t, sin_t = angle_tables(size, size, size)
    out = []
    for sign in (1.0, -1.0):
        high, low = halves_np(np.block([[cos_t, sign * sin_t], [-sign * sin_t, cos_t]]))
        out.append(np.concatenate([high, high, low], axis=1))
    return out


def col_matrices(size):
    cos_t, sin_t = angle_tables(size, size, size)
    out = []
    for sign in (1.0, -1.0):
        high, low = halves_np(np.block([[cos_t, -sign * sin_t], [sign * sin_t, cos_t]]))
        out.append(np.concatenate([high, high, low], axis=0))
    return out


def halves(value):
    high = value.astype(jnp.bfloat16)
    low = (value - high.astype(jnp.float32)).astype(jnp.bfloat16)
    return high, low


def fft_list(real, imag, sign):
    count = len(real)
    if count == 1:
        return real, imag
    even_r, even_i = fft_list(real[0::2], imag[0::2], sign)
    odd_r, odd_i = fft_list(real[1::2], imag[1::2], sign)
    half = count // 2
    out_r, out_i = [None] * count, [None] * count
    for k in range(half):
        cos_k = math.cos(2.0 * math.pi * k / count)
        sin_k = sign * math.sin(2.0 * math.pi * k / count)
        if k == 0:
            turn_r, turn_i = odd_r[k], odd_i[k]
        elif 4 * k == count:
            turn_r, turn_i = -sign * odd_i[k], sign * odd_r[k]
        else:
            turn_r = odd_r[k] * cos_k - odd_i[k] * sin_k
            turn_i = odd_r[k] * sin_k + odd_i[k] * cos_k
        out_r[k], out_i[k] = even_r[k] + turn_r, even_i[k] + turn_i
        out_r[k + half], out_i[k + half] = even_r[k] - turn_r, even_i[k] - turn_i
    return out_r, out_i


def dot_f32(left, right, dims):
    return lax.dot_general(left, right, (dims, ((), ())), preferred_element_type=jnp.float32)


def wide(row):
    return jnp.broadcast_to(row, (16, row.shape[1])).astype(jnp.bfloat16)


def one_hot_groups(index_rows, groups, cap):
    base = lax.broadcasted_iota(jnp.int32, (16, cap), 0).astype(jnp.float32)
    for group in groups:
        position = (base + float(16 * group)).astype(jnp.bfloat16)
        yield group, [position == row for row in index_rows]


def pick(hits, values):
    out = jnp.zeros(values[0].shape, values[0].dtype)
    for hit, value in zip(hits, values):
        out = jnp.where(hit, value, out)
    return out


def col_groups():
    return list(range(TC // 16 + 1)) + [WIN // 16 - 1]


def build_cols(geom, table_hi, table_lo):
    cap = geom.shape[1]
    weights = geom[8:12]
    high = weights.astype(jnp.bfloat16).astype(jnp.float32)
    low = weights - high
    index_rows = [wide(geom[16 + j : 17 + j]) for j in range(4)]
    high_rows = [wide(high[j : j + 1]) for j in range(4)]
    low_rows = [wide(low[j : j + 1]) for j in range(4)]
    for group, hits in one_hot_groups(index_rows, col_groups(), cap):
        at = pl.ds(16 * group, 16)
        table_hi[at, :] = pick(hits, high_rows)
        table_lo[at, :] = pick(hits, low_rows)


def build_rows(geom, vector, fold, table_hi, table_lo):
    cap = geom.shape[1]
    first, second = vector[0:1], vector[1:2]
    real = first * geom[0:4] + second * geom[4:8]
    imag = second * geom[0:4] - first * geom[4:8]
    index_rows = [wide(geom[12 + i : 13 + i]) for i in range(4)]
    rows = []
    for part in (real, imag):
        high = part.astype(jnp.bfloat16).astype(jnp.float32)
        low = part - high
        rows.append([wide(high[i : i + 1]) for i in range(4)])
        rows.append([wide(low[i : i + 1]) for i in range(4)])
    for group, hits in one_hot_groups(index_rows, range(fold // 16), cap):
        real_at = pl.ds(16 * group, 16)
        imag_at = pl.ds(fold + 16 * group, 16)
        table_hi[real_at, :] = pick(hits, rows[0])
        table_lo[real_at, :] = pick(hits, rows[1])
        table_hi[imag_at, :] = pick(hits, rows[2])
        table_lo[imag_at, :] = pick(hits, rows[3])


def spread_kernel(geom_ref, vec_ref, field_ref, acc, rhi0, rlo0, chi0, clo0, rhi1, rlo1, chi1, clo1):
    tiles, fold2, _ = field_ref.shape
    slabs = geom_ref.shape[0] // tiles
    fold = fold2 // 2
    for table in (chi0, clo0, chi1, clo1):
        table[...] = jnp.zeros(table.shape, table.dtype)
    field_ref[...] = jnp.zeros(field_ref.shape, jnp.float32)
    sets = ((rhi0, rlo0, chi0, clo0), (rhi1, rlo1, chi1, clo1))

    def per_tile(tile, carry):
        acc[...] = jnp.zeros(acc.shape, jnp.float32)

        def per_pair(pair, inner):
            for which in range(2):
                rhi, rlo, chi, clo = sets[which]
                at = (2 * pair + which) * tiles + tile
                geom = geom_ref[at]
                build_rows(geom, vec_ref[at], fold, rhi, rlo)
                build_cols(geom, chi, clo)
            for which in range(2):
                rhi, rlo, chi, clo = sets[which]
                left = jnp.concatenate([rhi[...], rlo[...], rhi[...]], axis=1)
                right = jnp.concatenate([chi[...], chi[...], clo[...]], axis=1)
                acc[...] += dot_f32(left, right, ((1,), (1,)))
            return inner

        lax.fori_loop(0, slabs // 2, per_pair, 0)
        lane = lax.broadcasted_iota(jnp.int32, (fold2, TC), 1)
        rim = acc[:, TC:]
        field_ref[tile] += acc[:, :TC]
        after = lax.rem(tile + 1, tiles)
        before = lax.rem(tile + tiles - 1, tiles)
        field_ref[after] += jnp.where(lane < TC // 2, rim, 0.0)
        field_ref[before] += jnp.where(lane < TC // 2, 0.0, rim)
        return carry

    lax.fori_loop(0, tiles, per_tile, 0)


def smooth_kernel(
    geom_ref, field_ref, spec_ref, row_fwd, row_inv, col_fwd, col_inv, turn_cos, turn_sin,
    out_ref, work, whi, wlo, chi0, clo0, chi1, clo1, blend0, blend1,
):
    tiles, fold2, _ = field_ref.shape
    fold = fold2 // 2
    slabs = geom_ref.shape[0] // tiles
    cap = geom_ref.shape[2]

    def rows_pass(matrix, source):
        def step(pair, carry):
            both = jnp.concatenate([source[2 * pair], source[2 * pair + 1]], axis=1)
            high, low = halves(both)
            stacked = jnp.concatenate([high, low, high], axis=0)
            result = dot_f32(matrix[...], stacked, ((1,), (0,)))
            work[2 * pair] = result[:, :TC]
            work[2 * pair + 1] = result[:, TC:]
            return carry

        lax.fori_loop(0, tiles // 2, step, 0)

    def tile_pass(sign):
        def step(group, carry):
            top = pl.multiple_of(8 * group, 8)
            real_at, imag_at = pl.ds(top, 8), pl.ds(fold + top, 8)
            real = [work[t, real_at, :] for t in range(tiles)]
            imag = [work[t, imag_at, :] for t in range(tiles)]

            def turned(real, imag):
                out_r, out_i = [], []
                for t in range(tiles):
                    cos_t, sin_t = turn_cos[t : t + 1, :], sign * turn_sin[t : t + 1, :]
                    out_r.append(real[t] * cos_t - imag[t] * sin_t)
                    out_i.append(real[t] * sin_t + imag[t] * cos_t)
                return out_r, out_i

            if sign < 0:
                real, imag = turned(*fft_list(real, imag, sign))
            else:
                real, imag = fft_list(*turned(real, imag), sign)
            for t in range(tiles):
                work[t, real_at, :] = real[t]
                work[t, imag_at, :] = imag[t]
            return carry

        lax.fori_loop(0, fold // 8, step, 0)

    def lane_pass():
        def product(left, matrix):
            high, low = halves(left)
            return dot_f32(jnp.concatenate([high, low, high], axis=1), matrix[...], ((1,), (0,)))

        def step(which, carry):
            left = jnp.concatenate([work[which, :fold, :], work[which, fold:, :]], axis=1)
            middle = product(left, col_fwd)
            spec = spec_ref[which].T
            middle = middle * jnp.concatenate([spec, spec], axis=1)
            result = product(middle, col_inv)
            work[which, :fold, :] = result[:, :TC]
            work[which, fold:, :] = result[:, TC:]
            return carry

        lax.fori_loop(0, tiles, step, 0)

    rows_pass(row_fwd, field_ref)
    tile_pass(-1.0)
    lane_pass()
    tile_pass(1.0)
    rows_pass(row_inv, work)

    sets = ((chi0, clo0, blend0), (chi1, clo1, blend1))
    for table in (chi0, clo0, chi1, clo1):
        table[...] = jnp.zeros(table.shape, table.dtype)

    def gathered(geom, blend):
        def row(at):
            return jnp.broadcast_to(geom[at : at + 1], (8, cap))

        cos_rows = [row(i) for i in range(4)]
        sin_rows = [row(4 + i) for i in range(4)]
        index_rows = [row(12 + i) for i in range(4)]
        base = lax.broadcasted_iota(jnp.int32, (8, cap), 0).astype(jnp.float32)
        first = jnp.zeros((8, cap), jnp.float32)
        second = jnp.zeros((8, cap), jnp.float32)
        for group in range(fold // 8):
            position = base + float(8 * group)
            hits = [position == index for index in index_rows]
            cos_t, sin_t = pick(hits, cos_rows), pick(hits, sin_rows)
            real = blend[8 * group : 8 * group + 8, :]
            imag = blend[fold + 8 * group : fold + 8 * group + 8, :]
            first = first + cos_t * real - sin_t * imag
            second = second + cos_t * imag + sin_t * real
        return jnp.concatenate(
            [jnp.sum(first, axis=0, keepdims=True), jnp.sum(second, axis=0, keepdims=True)], axis=0
        )

    def per_tile(tile, carry):
        lane = lax.broadcasted_iota(jnp.int32, (fold2, TC), 1)
        after = lax.rem(tile + 1, tiles)
        before = lax.rem(tile + tiles - 1, tiles)
        rim = jnp.where(lane < TC // 2, work[after], work[before])
        high, low = halves(jnp.concatenate([work[tile], rim], axis=1))
        whi[...] = high
        wlo[...] = low

        def per_pair(pair, inner):
            for which in range(2):
                chi, clo, blend = sets[which]
                at = (2 * pair + which) * tiles + tile
                build_cols(geom_ref[at], chi, clo)
                left = jnp.concatenate([whi[...], wlo[...], whi[...]], axis=1)
                right = jnp.concatenate([chi[...], chi[...], clo[...]], axis=0)
                blend[...] = dot_f32(left, right, ((1,), (0,)))
            for which in range(2):
                at = (2 * pair + which) * tiles + tile
                out_ref[at] = gathered(geom_ref[at], sets[which][2])
            return inner

        lax.fori_loop(0, slabs // 2, per_pair, 0)
        return carry

    lax.fori_loop(0, tiles, per_tile, 0)


def call_kernel(kernel, shape, scratch, args):
    vmem = pl.BlockSpec(memory_space=pltpu.VMEM)
    return pl.pallas_call(
        kernel,
        out_shape=jax.ShapeDtypeStruct(shape, jnp.float32),
        in_specs=[vmem] * len(args),
        out_specs=vmem,
        scratch_shapes=scratch,
        compiler_params=pltpu.CompilerParams(vmem_limit_bytes=VMEM_BYTES),
    )(*args)


def shared(value):
    count = lax.axis_size("slab")
    copies = jnp.broadcast_to(value[None], (count,) + value.shape)
    return lax.all_to_all(copies, "slab", 0, 0, tiled=True)


def geometry(cell_rows, cell_cols, fractions, fold):
    own = lax.axis_index("slab")
    slab = lax.broadcasted_iota(jnp.int32, cell_rows.shape, 0)
    row_weights = cubic_weights(fractions[0])
    col_weights = cubic_weights(fractions[1])
    parts = [[], [], [], [], []]
    for tap in range(4):
        row = (slab * fold + cell_rows - 1 + tap) % G
        angle = (own * row % G).astype(jnp.float32) * (2.0 * math.pi / G)
        parts[0].append(row_weights[tap] * jnp.cos(angle))
        parts[1].append(row_weights[tap] * jnp.sin(angle))
        parts[2].append(col_weights[tap])
        parts[3].append((row % fold).astype(jnp.float32))
        parts[4].append(((cell_cols - 1 + tap) % WIN).astype(jnp.float32))
    rows = sum(parts, [])
    rows = rows + [jnp.zeros_like(rows[0])] * (GEOM_ROWS - len(rows))
    stacked = jnp.stack(rows, axis=2)
    return stacked.reshape(-1, GEOM_ROWS, cell_rows.shape[2])


def spectrum_rows(spectrum, tiles, fold):
    slabs = lax.axis_size("slab")
    count = lax.axis_size("rhs")
    width = spectrum.shape[1]
    pieces = spectrum.reshape(fold, slabs, width).transpose(1, 2, 0) * (1.0 / (G * G))
    mine = lax.all_to_all(pieces, "slab", 0, 0, tiled=True)
    copies = jnp.broadcast_to(mine[None], (count,) + mine.shape)
    every = lax.all_to_all(copies, "rhs", 0, 0, tiled=True)
    columns = every.transpose(1, 0, 2, 3).reshape(G // tiles, tiles, fold)
    return columns.transpose(1, 0, 2)


def per_device(targets, counts, cell_rows, cell_cols, fractions, spectrum, noise_var):
    tiles, cap = cell_rows.shape
    slabs = lax.axis_size("slab")
    fold = G // slabs
    slot_index = lax.broadcasted_iota(jnp.int32, (tiles, cap), 1)
    live = (slot_index < counts[:, None]).astype(jnp.float32)[:, None, :]
    noise = noise_var[0]
    start = live * targets.transpose(1, 0, 2)

    payload = jnp.concatenate(
        [
            start,
            cell_rows.astype(jnp.float32)[:, None],
            cell_cols.astype(jnp.float32)[:, None],
            fractions.transpose(1, 0, 2),
        ],
        axis=1,
    )
    every = shared(payload)
    start_all = every[:, :, 0:2].reshape(slabs * tiles, 2, cap)
    geom = geometry(
        every[:, :, 2].astype(jnp.int32),
        every[:, :, 3].astype(jnp.int32),
        (every[:, :, 4], every[:, :, 5]),
        fold,
    )
    spec = spectrum_rows(spectrum, tiles, fold)
    row_fwd, row_inv = [jnp.asarray(m) for m in row_matrices(fold)]
    col_fwd, col_inv = [jnp.asarray(m) for m in col_matrices(TC)]
    turn_cos, turn_sin = [jnp.asarray(t.astype(np.float32)) for t in angle_tables(tiles, TC, G)]

    def vmem(shape, dtype):
        return pltpu.VMEM(shape, dtype)

    half = jnp.bfloat16
    row_tables = [vmem((2 * fold, cap), half)] * 2
    col_tables = [vmem((WIN, cap), half)] * 2

    def partial_product(vector):
        field = call_kernel(
            spread_kernel,
            (tiles, 2 * fold, TC),
            [vmem((2 * fold, WIN), jnp.float32)] + (row_tables + col_tables) * 2,
            (geom, vector),
        )
        return call_kernel(
            smooth_kernel,
            (slabs * tiles, 2, cap),
            [vmem((tiles, 2 * fold, TC), jnp.float32)]
            + [vmem((2 * fold, WIN), half)] * 2
            + col_tables * 2
            + [vmem((2 * fold, cap), jnp.float32)] * 2,
            (geom, field, spec, row_fwd, row_inv, col_fwd, col_inv, turn_cos, turn_sin),
        )

    def total(value):
        return jnp.sum(value, axis=(0, 2))

    def per_rhs(scale):
        return scale[None, :, None]

    direction_all = start_all
    residual_all = start_all
    direction = start
    residual = start
    solution = jnp.zeros_like(start)
    norm_now = total(start_all * start_all)
    for repeat in range(ITERS):
        partial = partial_product(direction_all)
        blocks = partial.reshape(slabs, tiles, 2, cap)
        if repeat + 1 < ITERS:
            smoothed = jnp.sum(lax.all_to_all(blocks, "slab", 0, 0, tiled=True), axis=0)
            image = live * smoothed + noise * direction
            image_all = shared(image).reshape(slabs * tiles, 2, cap)
            alpha = norm_now / total(direction_all * image_all)
            residual_all = residual_all - per_rhs(alpha) * image_all
            norm_next = total(residual_all * residual_all)
            beta = norm_next / norm_now
            solution = solution + per_rhs(alpha) * direction
            residual = residual - per_rhs(alpha) * image
            direction = residual + per_rhs(beta) * direction
            direction_all = residual_all + per_rhs(beta) * direction_all
            norm_now = norm_next
        else:
            share = total(direction_all * partial)
            extra = jnp.broadcast_to(share[None, None, :, None], (slabs, 1, 2, cap))
            blocks = jnp.concatenate([blocks, extra], axis=1)
            summed = jnp.sum(lax.all_to_all(blocks, "slab", 0, 0, tiled=True), axis=0)
            image = live * summed[:tiles] + noise * direction
            product = summed[tiles, :, 0] + noise * total(direction_all * direction_all)
            alpha = norm_now / product
            solution = solution + per_rhs(alpha) * direction
            residual = residual - per_rhs(alpha) * image
    return solution.transpose(1, 0, 2), residual.transpose(1, 0, 2)


def solution(mesh):
    placed = (
        P("rhs", "slab", None),
        P("slab"),
        P("slab", None),
        P("slab", None),
        P(None, "slab", None),
        P(None, ("slab", "rhs")),
        P(),
    )
    return jax.shard_map(
        per_device,
        mesh=mesh,
        in_specs=placed,
        out_specs=(P("rhs", "slab", None), P("rhs", "slab", None)),
        check_vma=False,
    )
```

```python
import math

import jax
import jax.numpy as jnp
import ml_dtypes
import numpy as np
from jax import lax
from jax.experimental import pallas as pl
from jax.experimental.pallas import tpu as pltpu
from jax.sharding import PartitionSpec as P

G = 2048
TC = 128
ITERS = 2
WIN = 2 * TC
GEOM_ROWS = 24
VMEM_BYTES = 60000 * 1024


def cubic_weights(fraction):
    return (
        ((-0.5 * fraction + 1.0) * fraction - 0.5) * fraction,
        (1.5 * fraction - 2.5) * fraction * fraction + 1.0,
        ((-1.5 * fraction + 2.0) * fraction + 0.5) * fraction,
        (0.5 * fraction - 0.5) * fraction * fraction,
    )


def halves_np(table):
    high = table.astype(np.float32).astype(ml_dtypes.bfloat16)
    low = (table - high.astype(np.float64)).astype(np.float32).astype(ml_dtypes.bfloat16)
    return high, low


def angle_tables(rows, cols, length):
    index = (np.arange(rows)[:, None] * np.arange(cols)[None, :]) % length
    angle = index * (2.0 * math.pi / length)
    return np.cos(angle), np.sin(angle)


def row_matrices(size):
    cos_t, sin_t = angle_tables(size, size, size)
    out = []
    for sign in (1.0, -1.0):
        high, low = halves_np(np.block([[cos_t, sign * sin_t], [-sign * sin_t, cos_t]]))
        out.append(np.concatenate([high, high, low], axis=1))
    return out


def col_matrices(size):
    cos_t, sin_t = angle_tables(size, size, size)
    out = []
    for sign in (1.0, -1.0):
        high, low = halves_np(np.block([[cos_t, -sign * sin_t], [sign * sin_t, cos_t]]))
        out.append(np.concatenate([high, high, low], axis=0))
    return out


def halves(value):
    high = value.astype(jnp.bfloat16)
    low = (value - high.astype(jnp.float32)).astype(jnp.bfloat16)
    return high, low


def fft_list(real, imag, sign):
    count = len(real)
    if count == 1:
        return real, imag
    even_r, even_i = fft_list(real[0::2], imag[0::2], sign)
    odd_r, odd_i = fft_list(real[1::2], imag[1::2], sign)
    half = count // 2
    out_r, out_i = [None] * count, [None] * count
    for k in range(half):
        cos_k = math.cos(2.0 * math.pi * k / count)
        sin_k = sign * math.sin(2.0 * math.pi * k / count)
        if k == 0:
            turn_r, turn_i = odd_r[k], odd_i[k]
        elif 4 * k == count:
            turn_r, turn_i = -sign * odd_i[k], sign * odd_r[k]
        else:
            turn_r = odd_r[k] * cos_k - odd_i[k] * sin_k
            turn_i = odd_r[k] * sin_k + odd_i[k] * cos_k
        out_r[k], out_i[k] = even_r[k] + turn_r, even_i[k] + turn_i
        out_r[k + half], out_i[k + half] = even_r[k] - turn_r, even_i[k] - turn_i
    return out_r, out_i


def dot_f32(left, right, dims):
    return lax.dot_general(left, right, (dims, ((), ())), preferred_element_type=jnp.float32)


def wide(row):
    return jnp.broadcast_to(row, (16, row.shape[1])).astype(jnp.bfloat16)


def pick(hits, values):
    out = jnp.zeros(values[0].shape, values[0].dtype)
    for hit, value in zip(hits, values):
        out = jnp.where(hit, value, out)
    return out


def patterns(inner, value_rows):
    position = lax.broadcasted_iota(jnp.int32, (16, inner.shape[1]), 0).astype(jnp.float32)
    here = [position.astype(jnp.bfloat16) == wide(inner + float(tap)) for tap in range(4)]
    there = [position.astype(jnp.bfloat16) == wide(inner + float(tap - 16)) for tap in range(4)]
    return [(pick(here, values), pick(there, values)) for values in value_rows]


def split_rows(part):
    high = part.astype(jnp.bfloat16).astype(jnp.float32)
    low = part - high
    return [[wide(half[i : i + 1]) for i in range(4)] for half in (high, low)]


def fill(block_row, groups, count, parts, stores):
    block = wide(block_row)
    for group, use_here, use_there in groups:
        here = block == jnp.bfloat16(group)
        there = block == jnp.bfloat16((group - 1) % count)
        for (part_here, part_there), store in zip(parts, stores):
            value = jnp.where(there, part_there, 0.0) if use_there else 0.0
            value = jnp.where(here, part_here, value) if use_here else value
            store(group, value.astype(jnp.bfloat16))


def store_in(table, top):
    def store(group, value):
        table[pl.ds(top + 16 * group, 16), :] = value

    return store


def build_cols(geom, table_hi, table_lo):
    inside = TC // 16
    count = WIN // 16
    groups = [(group, True, True) for group in range(inside)]
    groups += [(inside, False, True), (count - 1, True, False)]
    parts = patterns(geom[17:18], split_rows(geom[8:12]))
    fill(geom[16:17], groups, count, parts, (store_in(table_hi, 0), store_in(table_lo, 0)))


def build_rows(geom, vector, fold, table_hi, table_lo):
    first, second = vector[0:1], vector[1:2]
    real = first * geom[0:4] + second * geom[4:8]
    imag = second * geom[0:4] - first * geom[4:8]
    count = fold // 16
    parts = patterns(geom[13:14], split_rows(real) + split_rows(imag))
    stores = [store_in(table, top) for top in (0, fold) for table in (table_hi, table_lo)]
    fill(geom[12:13], [(group, True, True) for group in range(count)], count, parts, stores)


def place_all(chunks, offsets, block_at, tiles, slabs):
    cap = chunks.shape[3]
    step = math.gcd(slabs, 8)

    def some(count, carry):
        tile = count // (slabs // step)
        first = (count - tile * (slabs // step)) * step
        spots, turned = [], []
        for which in range(step):
            offset = offsets[(first + which) * tiles + tile]
            chunk = offset // cap
            shift = offset - chunk * cap
            spots.append((chunk, shift))
            turned.append(pltpu.roll(block_at(first + which, tile), shift, 1))
        lane = lax.broadcasted_iota(jnp.int32, turned[0].shape, 1)
        for (chunk, shift), block in zip(spots, turned):
            chunks[tile, chunk] = jnp.where(lane >= shift, block, chunks[tile, chunk])
            chunks[tile, chunk + 1] = jnp.where(lane < shift, block, 0.0)
        return carry

    lax.fori_loop(0, tiles * (slabs // step), some, 0)


def fetch_all(chunks, offsets, out_ref, tiles, slabs):
    cap = chunks.shape[3]
    step = math.gcd(slabs, 8)

    def some(count, carry):
        tile = count // (slabs // step)
        first = (count - tile * (slabs // step)) * step
        lane = lax.broadcasted_iota(jnp.int32, chunks.shape[2:], 1)
        turned = []
        for which in range(step):
            offset = offsets[(first + which) * tiles + tile]
            chunk = offset // cap
            shift = offset - chunk * cap
            both = jnp.where(lane >= shift, chunks[tile, chunk], chunks[tile, chunk + 1])
            turned.append(pltpu.roll(both, lax.rem(cap - shift, cap), 1))
        for which in range(step):
            out_ref[(first + which) * tiles + tile] = turned[which]
        return carry

    lax.fori_loop(0, tiles * (slabs // step), some, 0)


def circle(index):
    quarter = G // 4
    turn = (index + quarter // 2) // quarter
    x = (index - turn * quarter).astype(jnp.float32) * (2.0 * math.pi / G)
    y = x * x
    sin_x = 1.0 / 362880.0
    for term in (-1.0 / 5040.0, 1.0 / 120.0, -1.0 / 6.0, 1.0):
        sin_x = sin_x * y + term
    sin_x = sin_x * x
    cos_x = -1.0 / 3628800.0
    for term in (1.0 / 40320.0, -1.0 / 720.0, 1.0 / 24.0, -0.5, 1.0):
        cos_x = cos_x * y + term
    odd = (turn & 1) == 1
    cos_out = jnp.where(odd, sin_x, cos_x)
    sin_out = jnp.where(odd, cos_x, sin_x)
    cos_out = jnp.where(((turn + 1) & 2) == 2, -cos_out, cos_out)
    sin_out = jnp.where((turn & 2) == 2, -sin_out, sin_out)
    return cos_out, sin_out


def prepare_kernel(offsets, used, own, raw_ref, geom_ref, chunks):
    tiles, depth, _, cap = chunks.shape
    slabs = raw_ref.shape[0]
    fold = G // slabs
    chunks[...] = jnp.zeros(chunks.shape, jnp.float32)
    geom_ref[...] = jnp.zeros(geom_ref.shape, jnp.float32)
    place_all(chunks, offsets, lambda slab, tile: raw_ref[slab, tile], tiles, slabs)
    mine = own[0]
    steps = [circle((jnp.full((1, cap), tap, jnp.int32) * mine) & (G - 1)) for tap in range(1, 4)]

    def per_tile(tile, carry):
        def per_chunk(chunk, inner):
            raw = chunks[tile, chunk]
            row = jnp.maximum(raw[0:1].astype(jnp.int32), 0) + (G - 1)
            col = raw[1:2].astype(jnp.int32) + (WIN - 1)
            row_weights = cubic_weights(raw[2:3])
            col_weights = cubic_weights(raw[3:4])
            base_cos, base_sin = circle((row * mine) & (G - 1))
            for tap in range(4):
                cos_t, sin_t = base_cos, base_sin
                if tap:
                    step_cos, step_sin = steps[tap - 1]
                    cos_t = base_cos * step_cos - base_sin * step_sin
                    sin_t = base_sin * step_cos + base_cos * step_sin
                values = (row_weights[tap] * cos_t, row_weights[tap] * sin_t, col_weights[tap])
                for kind, value in enumerate(values):
                    at = 4 * kind + tap
                    geom_ref[tile, chunk, at : at + 1, :] = value
            row, col = row & (fold - 1), col & (WIN - 1)
            places = (row >> 4, row & 15, row >> 3, row & 7, col >> 4, col & 15)
            for kind, value in enumerate(places):
                at = 12 + kind
                geom_ref[tile, chunk, at : at + 1, :] = value.astype(jnp.float32)
            return inner

        lax.fori_loop(0, used[tile], per_chunk, 0)
        return carry

    lax.fori_loop(0, tiles, per_tile, 0)


def spread_kernel(offsets, used, geom_ref, vec_ref, field_ref, chunks, acc, rows0, cols0, rows1, cols1):
    tiles, fold2, _ = field_ref.shape
    slabs = vec_ref.shape[0] // tiles
    fold = fold2 // 2
    cap = chunks.shape[3]
    for table in (cols0, cols1):
        table[...] = jnp.zeros(table.shape, table.dtype)
    field_ref[...] = jnp.zeros(field_ref.shape, jnp.float32)
    chunks[...] = jnp.zeros(chunks.shape, jnp.float32)
    place_all(chunks, offsets, lambda slab, tile: vec_ref[slab * tiles + tile], tiles, slabs)
    sets = ((rows0, cols0), (rows1, cols1))

    def build(which, tile, chunk):
        rows, cols = sets[which]
        geom = geom_ref[tile, chunk]
        build_rows(geom, chunks[tile, chunk], fold, rows.at[0], rows.at[1])
        build_cols(geom, cols.at[0], cols.at[1])

    def add(which):
        rows, cols = sets[which]
        left = jnp.concatenate([rows[0], rows[1], rows[0]], axis=1)
        right = jnp.concatenate([cols[0], cols[0], cols[1]], axis=1)
        acc[...] += dot_f32(left, right, ((1,), (1,)))

    build(0, 0, 0)

    def per_tile(tile, carry):
        acc[...] = jnp.zeros(acc.shape, jnp.float32)
        pairs = (used[tile] + 1) // 2

        def per_pair(pair, inner):
            last = pair + 1 == pairs
            add(0)
            build(1, tile, 2 * pair + 1)
            add(1)
            build(
                0,
                jnp.where(last, jnp.minimum(tile + 1, tiles - 1), tile),
                jnp.where(last, 0, 2 * pair + 2),
            )
            return inner

        lax.fori_loop(0, pairs, per_pair, 0)
        lane = lax.broadcasted_iota(jnp.int32, (fold2, TC), 1)
        rim = acc[:, TC:]
        field_ref[tile] += acc[:, :TC]
        after = lax.rem(tile + 1, tiles)
        before = lax.rem(tile + tiles - 1, tiles)
        field_ref[after] += jnp.where(lane < TC // 2, rim, 0.0)
        field_ref[before] += jnp.where(lane < TC // 2, 0.0, rim)
        return carry

    lax.fori_loop(0, tiles, per_tile, 0)


def smooth_kernel(
    offsets, used, geom_ref, field_ref, spec_ref, row_fwd, row_inv, col_fwd, col_inv, turn_cos, turn_sin,
    out_ref, work, whi, wlo, cols0, cols1, chunks, blend0, blend1,
):
    tiles, fold2, _ = field_ref.shape
    fold = fold2 // 2
    slabs = out_ref.shape[0] // tiles
    cap = geom_ref.shape[3]

    def rows_pass(matrix, source):
        def step(pair, carry):
            both = jnp.concatenate([source[2 * pair], source[2 * pair + 1]], axis=1)
            high, low = halves(both)
            stacked = jnp.concatenate([high, low, high], axis=0)
            result = dot_f32(matrix[...], stacked, ((1,), (0,)))
            work[2 * pair] = result[:, :TC]
            work[2 * pair + 1] = result[:, TC:]
            return carry

        lax.fori_loop(0, tiles // 2, step, 0)

    def tile_pass(sign):
        def step(group, carry):
            top = pl.multiple_of(8 * group, 8)
            real_at, imag_at = pl.ds(top, 8), pl.ds(fold + top, 8)
            real = [work[t, real_at, :] for t in range(tiles)]
            imag = [work[t, imag_at, :] for t in range(tiles)]

            def turned(real, imag):
                out_r, out_i = [], []
                for t in range(tiles):
                    cos_t, sin_t = turn_cos[t : t + 1, :], sign * turn_sin[t : t + 1, :]
                    out_r.append(real[t] * cos_t - imag[t] * sin_t)
                    out_i.append(real[t] * sin_t + imag[t] * cos_t)
                return out_r, out_i

            if sign < 0:
                real, imag = turned(*fft_list(real, imag, sign))
            else:
                real, imag = fft_list(*turned(real, imag), sign)
            for t in range(tiles):
                work[t, real_at, :] = real[t]
                work[t, imag_at, :] = imag[t]
            return carry

        lax.fori_loop(0, fold // 8, step, 0)

    def lane_pass():
        def product(left, matrix):
            high, low = halves(left)
            return dot_f32(jnp.concatenate([high, low, high], axis=1), matrix[...], ((1,), (0,)))

        def step(which, carry):
            left = jnp.concatenate([work[which, :fold, :], work[which, fold:, :]], axis=1)
            middle = product(left, col_fwd)
            spec = spec_ref[which].T
            middle = middle * jnp.concatenate([spec, spec], axis=1)
            result = product(middle, col_inv)
            work[which, :fold, :] = result[:, :TC]
            work[which, fold:, :] = result[:, TC:]
            return carry

        lax.fori_loop(0, tiles, step, 0)

    rows_pass(row_fwd, field_ref)
    tile_pass(-1.0)
    lane_pass()
    tile_pass(1.0)
    rows_pass(row_inv, work)

    sets = ((cols0, blend0), (cols1, blend1))
    blend1[...] = jnp.zeros(blend1.shape, jnp.float32)
    for table in (cols0, cols1):
        table[...] = jnp.zeros(table.shape, table.dtype)
    chunks[...] = jnp.zeros(chunks.shape, jnp.float32)

    def gathered(geom, blend):
        block = jnp.broadcast_to(geom[14:15], (8, cap))
        count = fold // 8
        zero = jnp.zeros((8, cap), jnp.float32)
        here = [zero, zero]
        there = [zero, zero]
        for group in range(count):
            hit = block == float(group)
            for part in range(2):
                top = part * fold + 8 * group
                after = part * fold + 8 * ((group + 1) % count)
                here[part] = jnp.where(hit, blend[top : top + 8, :], here[part])
                there[part] = jnp.where(hit, blend[after : after + 8, :], there[part])
        position = lax.broadcasted_iota(jnp.int32, (8, cap), 0).astype(jnp.float32)
        first, second = zero, zero
        for shift, (real, imag) in ((0.0, here), (8.0, there)):
            hits = [position == geom[15:16] + (tap - shift) for tap in range(4)]
            cos_t = pick(hits, [jnp.broadcast_to(geom[i : i + 1], (8, cap)) for i in range(4)])
            sin_t = pick(hits, [jnp.broadcast_to(geom[4 + i : 5 + i], (8, cap)) for i in range(4)])
            first = first + cos_t * real - sin_t * imag
            second = second + cos_t * imag + sin_t * real
        return jnp.sum(first, axis=0, keepdims=True), jnp.sum(second, axis=0, keepdims=True)

    def start_blend(which, tile, chunk):
        cols, blend = sets[which]
        build_cols(geom_ref[tile, chunk], cols.at[0], cols.at[1])
        left = jnp.concatenate([whi[...], wlo[...], whi[...]], axis=1)
        right = jnp.concatenate([cols[0], cols[0], cols[1]], axis=0)
        blend[...] = dot_f32(left, right, ((1,), (0,)))

    def finish(which, tile, chunk):
        first, second = gathered(geom_ref[tile, chunk], sets[which][1])
        chunks[tile, chunk, 0:1, :] = first
        chunks[tile, chunk, 1:2, :] = second

    def per_tile(tile, last):
        lane = lax.broadcasted_iota(jnp.int32, (fold2, TC), 1)
        after = lax.rem(tile + 1, tiles)
        before = lax.rem(tile + tiles - 1, tiles)
        rim = jnp.where(lane < TC // 2, work[after], work[before])
        high, low = halves(jnp.concatenate([work[tile], rim], axis=1))
        whi[...] = high
        wlo[...] = low

        def per_pair(pair, last):
            start_blend(0, tile, 2 * pair)
            finish(1, *last)
            start_blend(1, tile, 2 * pair + 1)
            finish(0, tile, 2 * pair)
            return tile, 2 * pair + 1

        return lax.fori_loop(0, (used[tile] + 1) // 2, per_pair, last)

    spare = chunks.shape[1] - 1
    finish(1, *lax.fori_loop(0, tiles, per_tile, (0, spare)))
    fetch_all(chunks, offsets, out_ref, tiles, slabs)


def call_kernel(kernel, shape, scratch, scalars, args):
    vmem = pl.BlockSpec(memory_space=pltpu.VMEM)
    smem = pl.BlockSpec(memory_space=pltpu.SMEM)
    return pl.pallas_call(
        kernel,
        out_shape=jax.ShapeDtypeStruct(shape, jnp.float32),
        in_specs=[smem] * len(scalars) + [vmem] * len(args),
        out_specs=vmem,
        scratch_shapes=scratch,
        compiler_params=pltpu.CompilerParams(vmem_limit_bytes=VMEM_BYTES),
        cost_estimate=pl.CostEstimate(flops=4 * 10**9, bytes_accessed=10**7, transcendentals=0),
    )(*scalars, *args)


def shared(value):
    count = lax.axis_size("slab")
    copies = jnp.broadcast_to(value[None], (count,) + value.shape)
    return lax.all_to_all(copies, "slab", 0, 0, tiled=True)


def spectrum_slab(spectrum, fold):
    pieces = spectrum.reshape(fold, G // fold, -1).transpose(1, 2, 0) * (1.0 / (G * G))
    return lax.all_to_all(pieces, "slab", 0, 0, tiled=True)


def spectrum_rows(mine, tiles, fold):
    count = lax.axis_size("rhs")
    copies = jnp.broadcast_to(mine[None], (count,) + mine.shape)
    every = lax.all_to_all(copies, "rhs", 0, 0, tiled=True)
    columns = every.transpose(1, 0, 2, 3).reshape(G // tiles, tiles, fold)
    return columns.transpose(1, 0, 2)


def per_device(targets, counts, cell_rows, cell_cols, fractions, spectrum, noise_var):
    tiles, cap = cell_rows.shape
    slabs = lax.axis_size("slab")
    fold = G // slabs
    slot_index = lax.broadcasted_iota(jnp.int32, (tiles, cap), 1)
    live = (slot_index < counts[:, None]).astype(jnp.float32)[:, None, :]
    noise = noise_var[0]
    start = live * targets.transpose(1, 0, 2)

    own = lax.axis_index("slab").astype(jnp.int32).reshape(1)
    rows = jnp.where(live > 0, (own[0] * fold + cell_rows).astype(jnp.float32)[:, None], -1.0)
    payload = jnp.concatenate(
        [rows, cell_cols.astype(jnp.float32)[:, None], fractions.transpose(1, 0, 2), start], axis=1
    )
    every = shared(payload.reshape(-1, cap)).reshape((slabs,) + payload.shape)
    every, spectrum = lax.optimization_barrier((every, spectrum))
    start_all = every[:, :, 4:6].reshape(slabs * tiles, 2, cap)
    filled = jnp.sum((every[:, :, 0] >= 0.0).astype(jnp.int32), axis=2)
    before = [jnp.zeros((tiles,), jnp.int32)]
    for slab in range(slabs):
        before.append(before[-1] + filled[slab])
    offsets = jnp.concatenate(before[:-1])
    used = (before[-1] + (cap - 1)) // cap
    depth = slabs + 2
    geom = call_kernel(
        prepare_kernel,
        (tiles, depth, GEOM_ROWS, cap),
        [pltpu.VMEM((tiles, depth, every.shape[2], cap), jnp.float32)],
        (offsets, used, own),
        (every,),
    )
    mine = spectrum_slab(spectrum, fold)
    geom, mine = lax.optimization_barrier((geom, mine))
    spec = spectrum_rows(mine, tiles, fold)
    row_fwd, row_inv = [jnp.asarray(m) for m in row_matrices(fold)]
    col_fwd, col_inv = [jnp.asarray(m) for m in col_matrices(TC)]
    turn_cos, turn_sin = [jnp.asarray(t.astype(np.float32)) for t in angle_tables(tiles, TC, G)]

    def vmem(shape, dtype):
        return pltpu.VMEM(shape, dtype)

    half = jnp.bfloat16
    row_table = vmem((2, 2 * fold, cap), half)
    col_table = vmem((2, WIN, cap), half)
    point_chunks = vmem((tiles, depth, 2, cap), jnp.float32)

    def partial_product(vector):
        field = call_kernel(
            spread_kernel,
            (tiles, 2 * fold, TC),
            [point_chunks, vmem((2 * fold, WIN), jnp.float32)] + [row_table, col_table] * 2,
            (offsets, used),
            (geom, vector),
        )
        return call_kernel(
            smooth_kernel,
            (slabs * tiles, 2, cap),
            [vmem((tiles, 2 * fold, TC), jnp.float32)]
            + [vmem((2 * fold, WIN), half)] * 2
            + [col_table] * 2
            + [point_chunks]
            + [vmem((2 * fold, cap), jnp.float32)] * 2,
            (offsets, used),
            (geom, field, spec, row_fwd, row_inv, col_fwd, col_inv, turn_cos, turn_sin),
        )

    def total(value):
        return jnp.sum(value, axis=(0, 2))

    def per_rhs(scale):
        return scale[None, :, None]

    direction_all = start_all
    residual_all = start_all
    direction = start
    residual = start
    solution = jnp.zeros_like(start)
    norm_now = total(start_all * start_all)
    for repeat in range(ITERS):
        partial = partial_product(direction_all)
        blocks = partial.reshape(slabs, tiles, 2, cap)
        if repeat + 1 < ITERS:
            smoothed = jnp.sum(lax.all_to_all(blocks, "slab", 0, 0, tiled=True), axis=0)
            image = live * smoothed + noise * direction
            image_all = shared(image).reshape(slabs * tiles, 2, cap)
            alpha = norm_now / total(direction_all * image_all)
            residual_all = residual_all - per_rhs(alpha) * image_all
            norm_next = total(residual_all * residual_all)
            beta = norm_next / norm_now
            solution = solution + per_rhs(alpha) * direction
            residual = residual - per_rhs(alpha) * image
            direction = residual + per_rhs(beta) * direction
            direction_all = residual_all + per_rhs(beta) * direction_all
            norm_now = norm_next
        else:
            share = total(direction_all * partial)
            extra = jnp.broadcast_to(share[None, None, :, None], (slabs, 1, 2, cap))
            blocks = jnp.concatenate([blocks, extra], axis=1)
            summed = jnp.sum(lax.all_to_all(blocks, "slab", 0, 0, tiled=True), axis=0)
            image = live * summed[:tiles] + noise * direction
            product = summed[tiles, :, 0] + noise * total(direction_all * direction_all)
            alpha = norm_now / product
            solution = solution + per_rhs(alpha) * direction
            residual = residual - per_rhs(alpha) * image
    return solution.transpose(1, 0, 2), residual.transpose(1, 0, 2)


def solution(mesh):
    placed = (
        P("rhs", "slab", None),
        P("slab"),
        P("slab", None),
        P("slab", None),
        P(None, "slab", None),
        P(None, ("slab", "rhs")),
        P(),
    )
    return jax.shard_map(
        per_device,
        mesh=mesh,
        in_specs=placed,
        out_specs=(P("rhs", "slab", None), P("rhs", "slab", None)),
        check_vma=False,
    )
```

```python
import math

import jax
import jax.numpy as jnp
import ml_dtypes
import numpy as np
from jax import lax
from jax.experimental import pallas as pl
from jax.experimental.pallas import tpu as pltpu
from jax.sharding import PartitionSpec as P

G = 2048
TC = 128
ITERS = 2
WIN = 2 * TC
GEOM_ROWS = 24
VMEM_BYTES = 30 * 1024 * 1024


def cubic_weights(fraction):
    return (
        ((-0.5 * fraction + 1.0) * fraction - 0.5) * fraction,
        (1.5 * fraction - 2.5) * fraction * fraction + 1.0,
        ((-1.5 * fraction + 2.0) * fraction + 0.5) * fraction,
        (0.5 * fraction - 0.5) * fraction * fraction,
    )


def halves_np(table):
    high = table.astype(np.float32).astype(ml_dtypes.bfloat16)
    low = (table - high.astype(np.float64)).astype(np.float32).astype(ml_dtypes.bfloat16)
    return high, low


def angle_tables(rows, cols, length):
    index = (np.arange(rows)[:, None] * np.arange(cols)[None, :]) % length
    angle = index * (2.0 * math.pi / length)
    return np.cos(angle), np.sin(angle)


def row_matrices(size):
    cos_t, sin_t = angle_tables(size, size, size)
    out = []
    for sign in (1.0, -1.0):
        high, low = halves_np(np.block([[cos_t, sign * sin_t], [-sign * sin_t, cos_t]]))
        out.append(np.concatenate([high, high, low], axis=1))
    return out


def col_matrices(size):
    cos_t, sin_t = angle_tables(size, size, size)
    out = []
    for sign in (1.0, -1.0):
        high, low = halves_np(np.block([[cos_t, -sign * sin_t], [sign * sin_t, cos_t]]))
        out.append(np.concatenate([high, high, low], axis=0))
    return out


def halves(value):
    high = value.astype(jnp.bfloat16)
    low = (value - high.astype(jnp.float32)).astype(jnp.bfloat16)
    return high, low


def fft_list(real, imag, sign):
    count = len(real)
    if count == 1:
        return real, imag
    even_r, even_i = fft_list(real[0::2], imag[0::2], sign)
    odd_r, odd_i = fft_list(real[1::2], imag[1::2], sign)
    half = count // 2
    out_r, out_i = [None] * count, [None] * count
    for k in range(half):
        cos_k = math.cos(2.0 * math.pi * k / count)
        sin_k = sign * math.sin(2.0 * math.pi * k / count)
        if k == 0:
            turn_r, turn_i = odd_r[k], odd_i[k]
        elif 4 * k == count:
            turn_r, turn_i = -sign * odd_i[k], sign * odd_r[k]
        else:
            turn_r = odd_r[k] * cos_k - odd_i[k] * sin_k
            turn_i = odd_r[k] * sin_k + odd_i[k] * cos_k
        out_r[k], out_i[k] = even_r[k] + turn_r, even_i[k] + turn_i
        out_r[k + half], out_i[k + half] = even_r[k] - turn_r, even_i[k] - turn_i
    return out_r, out_i


def dot_f32(left, right, dims):
    return lax.dot_general(left, right, (dims, ((), ())), preferred_element_type=jnp.float32)


def wide(row):
    return jnp.broadcast_to(row, (16, row.shape[1])).astype(jnp.bfloat16)


def pick(hits, values):
    out = jnp.zeros(values[0].shape, values[0].dtype)
    for hit, value in zip(hits, values):
        out = jnp.where(hit, value, out)
    return out


def patterns(inner, value_rows):
    position = lax.broadcasted_iota(jnp.int32, (16, inner.shape[1]), 0).astype(jnp.float32)
    here = [position.astype(jnp.bfloat16) == wide(inner + float(tap)) for tap in range(4)]
    there = [position.astype(jnp.bfloat16) == wide(inner + float(tap - 16)) for tap in range(4)]
    return [(pick(here, values), pick(there, values)) for values in value_rows]


def split_rows(part):
    high = part.astype(jnp.bfloat16).astype(jnp.float32)
    low = part - high
    return [[wide(half[i : i + 1]) for i in range(4)] for half in (high, low)]


def fill(block_row, groups, count, parts, stores):
    block = wide(block_row)
    for group, use_here, use_there in groups:
        here = block == jnp.bfloat16(group)
        there = block == jnp.bfloat16((group - 1) % count)
        for (part_here, part_there), store in zip(parts, stores):
            value = jnp.where(there, part_there, 0.0) if use_there else 0.0
            value = jnp.where(here, part_here, value) if use_here else value
            store(group, value.astype(jnp.bfloat16))


def store_in(table, top):
    def store(group, value):
        table[pl.ds(top + 16 * group, 16), :] = value

    return store


def build_cols(geom, table_hi, table_lo):
    inside = TC // 16
    count = WIN // 16
    groups = [(group, True, True) for group in range(inside)]
    groups += [(inside, False, True), (count - 1, True, False)]
    parts = patterns(geom[17:18], split_rows(geom[8:12]))
    fill(geom[16:17], groups, count, parts, (store_in(table_hi, 0), store_in(table_lo, 0)))


def build_rows(geom, vector, fold, table_hi, table_lo):
    first, second = vector[0:1], vector[1:2]
    real = first * geom[0:4] + second * geom[4:8]
    imag = second * geom[0:4] - first * geom[4:8]
    count = fold // 16
    parts = patterns(geom[13:14], split_rows(real) + split_rows(imag))
    stores = [store_in(table, top) for top in (0, fold) for table in (table_hi, table_lo)]
    fill(geom[12:13], [(group, True, True) for group in range(count)], count, parts, stores)


def place_all(chunks, offsets, block_at, tiles, slabs):
    cap = chunks.shape[3]
    step = math.gcd(slabs, 8)

    def some(count, carry):
        tile = count // (slabs // step)
        first = (count - tile * (slabs // step)) * step
        spots, turned = [], []
        for which in range(step):
            offset = offsets[(first + which) * tiles + tile]
            chunk = offset // cap
            shift = offset - chunk * cap
            spots.append((chunk, shift))
            turned.append(pltpu.roll(block_at(first + which, tile), shift, 1))
        lane = lax.broadcasted_iota(jnp.int32, turned[0].shape, 1)
        for (chunk, shift), block in zip(spots, turned):
            chunks[tile, chunk] = jnp.where(lane >= shift, block, chunks[tile, chunk])
            chunks[tile, chunk + 1] = jnp.where(lane < shift, block, 0.0)
        return carry

    lax.fori_loop(0, tiles * (slabs // step), some, 0)


def fetch_all(chunks, offsets, out_ref, tiles, slabs):
    cap = chunks.shape[3]
    step = math.gcd(slabs, 8)

    def some(count, carry):
        tile = count // (slabs // step)
        first = (count - tile * (slabs // step)) * step
        lane = lax.broadcasted_iota(jnp.int32, chunks.shape[2:], 1)
        turned = []
        for which in range(step):
            offset = offsets[(first + which) * tiles + tile]
            chunk = offset // cap
            shift = offset - chunk * cap
            both = jnp.where(lane >= shift, chunks[tile, chunk], chunks[tile, chunk + 1])
            turned.append(pltpu.roll(both, lax.rem(cap - shift, cap), 1))
        for which in range(step):
            out_ref[(first + which) * tiles + tile] = turned[which]
        return carry

    lax.fori_loop(0, tiles * (slabs // step), some, 0)


def circle(index):
    quarter = G // 4
    turn = (index + quarter // 2) // quarter
    x = (index - turn * quarter).astype(jnp.float32) * (2.0 * math.pi / G)
    y = x * x
    sin_x = 1.0 / 362880.0
    for term in (-1.0 / 5040.0, 1.0 / 120.0, -1.0 / 6.0, 1.0):
        sin_x = sin_x * y + term
    sin_x = sin_x * x
    cos_x = -1.0 / 3628800.0
    for term in (1.0 / 40320.0, -1.0 / 720.0, 1.0 / 24.0, -0.5, 1.0):
        cos_x = cos_x * y + term
    odd = (turn & 1) == 1
    cos_out = jnp.where(odd, sin_x, cos_x)
    sin_out = jnp.where(odd, cos_x, sin_x)
    cos_out = jnp.where(((turn + 1) & 2) == 2, -cos_out, cos_out)
    sin_out = jnp.where((turn & 2) == 2, -sin_out, sin_out)
    return cos_out, sin_out


def prepare_kernel(offsets, used, own, raw_ref, geom_ref, chunks):
    tiles, depth, _, cap = chunks.shape
    slabs = raw_ref.shape[0]
    fold = G // slabs
    chunks[...] = jnp.zeros(chunks.shape, jnp.float32)
    geom_ref[...] = jnp.zeros(geom_ref.shape, jnp.float32)
    place_all(chunks, offsets, lambda slab, tile: raw_ref[slab, tile], tiles, slabs)
    mine = own[0]
    steps = [circle((jnp.full((1, cap), tap, jnp.int32) * mine) & (G - 1)) for tap in range(1, 4)]

    def per_tile(tile, carry):
        def per_chunk(chunk, inner):
            raw = chunks[tile, chunk]
            row = jnp.maximum(raw[0:1].astype(jnp.int32), 0) + (G - 1)
            col = raw[1:2].astype(jnp.int32) + (WIN - 1)
            row_weights = cubic_weights(raw[2:3])
            col_weights = cubic_weights(raw[3:4])
            base_cos, base_sin = circle((row * mine) & (G - 1))
            for tap in range(4):
                cos_t, sin_t = base_cos, base_sin
                if tap:
                    step_cos, step_sin = steps[tap - 1]
                    cos_t = base_cos * step_cos - base_sin * step_sin
                    sin_t = base_sin * step_cos + base_cos * step_sin
                values = (row_weights[tap] * cos_t, row_weights[tap] * sin_t, col_weights[tap])
                for kind, value in enumerate(values):
                    at = 4 * kind + tap
                    geom_ref[tile, chunk, at : at + 1, :] = value
            row, col = row & (fold - 1), col & (WIN - 1)
            places = (row >> 4, row & 15, row >> 3, row & 7, col >> 4, col & 15)
            for kind, value in enumerate(places):
                at = 12 + kind
                geom_ref[tile, chunk, at : at + 1, :] = value.astype(jnp.float32)
            return inner

        lax.fori_loop(0, used[tile], per_chunk, 0)
        return carry

    lax.fori_loop(0, tiles, per_tile, 0)


def spread_kernel(offsets, used, geom_ref, vec_ref, field_ref, chunks, acc, rows0, cols0, rows1, cols1):
    tiles, fold2, _ = field_ref.shape
    slabs = vec_ref.shape[0] // tiles
    fold = fold2 // 2
    cap = chunks.shape[3]
    for table in (cols0, cols1):
        table[...] = jnp.zeros(table.shape, table.dtype)
    field_ref[...] = jnp.zeros(field_ref.shape, jnp.float32)
    chunks[...] = jnp.zeros(chunks.shape, jnp.float32)
    place_all(chunks, offsets, lambda slab, tile: vec_ref[slab * tiles + tile], tiles, slabs)
    sets = ((rows0, cols0), (rows1, cols1))

    def build(which, tile, chunk):
        rows, cols = sets[which]
        geom = geom_ref[tile, chunk]
        build_rows(geom, chunks[tile, chunk], fold, rows.at[0], rows.at[1])
        build_cols(geom, cols.at[0], cols.at[1])

    def add(which):
        rows, cols = sets[which]
        left = jnp.concatenate([rows[0], rows[1], rows[0]], axis=1)
        right = jnp.concatenate([cols[0], cols[0], cols[1]], axis=1)
        acc[...] += dot_f32(left, right, ((1,), (1,)))

    build(0, 0, 0)

    def per_tile(tile, carry):
        acc[...] = jnp.zeros(acc.shape, jnp.float32)
        behind = jnp.minimum(tile + 1, tiles - 1)

        def per_pair(pair, inner):
            more = 2 * pair + 2 < used[tile]
            add(0)
            build(1, tile, 2 * pair + 1)
            add(1)
            build(0, jnp.where(more, tile, behind), jnp.where(more, 2 * pair + 2, 0))
            return inner

        lax.fori_loop(0, used[tile] // 2, per_pair, 0)

        @pl.when(lax.rem(used[tile], 2) == 1)
        def _():
            add(0)
            build(0, behind, 0)

        lane = lax.broadcasted_iota(jnp.int32, (fold2, TC), 1)
        rim = acc[:, TC:]
        field_ref[tile] += acc[:, :TC]
        after = lax.rem(tile + 1, tiles)
        before = lax.rem(tile + tiles - 1, tiles)
        field_ref[after] += jnp.where(lane < TC // 2, rim, 0.0)
        field_ref[before] += jnp.where(lane < TC // 2, 0.0, rim)
        return carry

    lax.fori_loop(0, tiles, per_tile, 0)


def smooth_kernel(
    offsets, used, geom_ref, field_ref, spec_ref, row_fwd, row_inv, col_fwd, col_inv,
    turn_cos, turn_sin, mix_cos, mix_sin, out_ref, work, whi, wlo, cols0, cols1, chunks, blend0, blend1,
):
    tiles, fold2, _ = field_ref.shape
    fold = fold2 // 2
    slabs = out_ref.shape[0] // tiles
    cap = geom_ref.shape[3]

    half = fold // 2
    many = math.gcd(tiles, 4)

    def product_rows(matrix, columns):
        high, low = halves(jnp.concatenate(columns, axis=1))
        result = dot_f32(matrix[...], jnp.concatenate([high, low, high], axis=0), ((1,), (0,)))
        return [result[:, TC * i : TC * (i + 1)] for i in range(len(columns))]

    def rows_forward(group, carry):
        columns = []
        for which in range(many):
            block = field_ref[many * group + which]
            real_a, real_b = block[:half], block[half:fold]
            imag_a, imag_b = block[fold : fold + half], block[fold + half :]
            real_d, imag_d = real_a - real_b, imag_a - imag_b
            columns.append(jnp.concatenate([real_a + real_b, imag_a + imag_b], axis=0))
            columns.append(
                jnp.concatenate(
                    [
                        real_d * mix_cos[...] + imag_d * mix_sin[...],
                        imag_d * mix_cos[...] - real_d * mix_sin[...],
                    ],
                    axis=0,
                )
            )
        results = product_rows(row_fwd, columns)
        for which in range(many):
            for odd in range(2):
                result = results[2 * which + odd]
                at = odd * half
                work[many * group + which, at : at + half, :] = result[:half]
                work[many * group + which, fold + at : fold + at + half, :] = result[half:]
        return carry

    def rows_inverse(group, carry):
        columns = []
        for which in range(many):
            block = work[many * group + which]
            columns.append(jnp.concatenate([block[:half], block[fold : fold + half]], axis=0))
            columns.append(jnp.concatenate([block[half:fold], block[fold + half :]], axis=0))
        results = product_rows(row_inv, columns)
        for which in range(many):
            even, odd = results[2 * which], results[2 * which + 1]
            real_t = odd[:half] * mix_cos[...] - odd[half:] * mix_sin[...]
            imag_t = odd[:half] * mix_sin[...] + odd[half:] * mix_cos[...]
            at = many * group + which
            work[at, :half, :] = even[:half] + real_t
            work[at, half:fold, :] = even[:half] - real_t
            work[at, fold : fold + half, :] = even[half:] + imag_t
            work[at, fold + half :, :] = even[half:] - imag_t
        return carry

    def tile_pass(sign):
        def step(group, carry):
            top = pl.multiple_of(8 * group, 8)
            real_at, imag_at = pl.ds(top, 8), pl.ds(fold + top, 8)
            real = [work[t, real_at, :] for t in range(tiles)]
            imag = [work[t, imag_at, :] for t in range(tiles)]

            def turned(real, imag):
                out_r, out_i = [], []
                for t in range(tiles):
                    cos_t, sin_t = turn_cos[t : t + 1, :], sign * turn_sin[t : t + 1, :]
                    out_r.append(real[t] * cos_t - imag[t] * sin_t)
                    out_i.append(real[t] * sin_t + imag[t] * cos_t)
                return out_r, out_i

            if sign < 0:
                real, imag = turned(*fft_list(real, imag, sign))
            else:
                real, imag = fft_list(*turned(real, imag), sign)
            for t in range(tiles):
                work[t, real_at, :] = real[t]
                work[t, imag_at, :] = imag[t]
            return carry

        lax.fori_loop(0, fold // 8, step, 0)

    def lane_pass():
        def product(left, matrix):
            high, low = halves(left)
            return dot_f32(jnp.concatenate([high, low, high], axis=1), matrix[...], ((1,), (0,)))

        def step(group, carry):
            ats = [many * group + which for which in range(many)]
            left = jnp.concatenate(
                [jnp.concatenate([work[at, :fold, :], work[at, fold:, :]], axis=1) for at in ats], axis=0
            )
            middle = product(left, col_fwd)
            spec = jnp.concatenate([spec_ref[at].T for at in ats], axis=0)
            middle = middle * jnp.concatenate([spec, spec], axis=1)
            result = product(middle, col_inv)
            for which, at in enumerate(ats):
                part = result[fold * which : fold * (which + 1)]
                work[at, :fold, :] = part[:, :TC]
                work[at, fold:, :] = part[:, TC:]
            return carry

        lax.fori_loop(0, tiles // many, step, 0)

    lax.fori_loop(0, tiles // many, rows_forward, 0)
    tile_pass(-1.0)
    lane_pass()
    tile_pass(1.0)
    lax.fori_loop(0, tiles // many, rows_inverse, 0)

    sets = ((cols0, blend0), (cols1, blend1))
    blend1[...] = jnp.zeros(blend1.shape, jnp.float32)
    for table in (cols0, cols1):
        table[...] = jnp.zeros(table.shape, table.dtype)
    chunks[...] = jnp.zeros(chunks.shape, jnp.float32)

    def gathered(geom, blend):
        block = jnp.broadcast_to(geom[14:15], (8, cap))
        count = fold // 8
        zero = jnp.zeros((8, cap), jnp.float32)
        here = [zero, zero]
        there = [zero, zero]
        for group in range(count):
            hit = block == float(group)
            for part in range(2):
                top = part * fold + 8 * group
                after = part * fold + 8 * ((group + 1) % count)
                here[part] = jnp.where(hit, blend[top : top + 8, :], here[part])
                there[part] = jnp.where(hit, blend[after : after + 8, :], there[part])
        position = lax.broadcasted_iota(jnp.int32, (8, cap), 0).astype(jnp.float32)
        first, second = zero, zero
        for shift, (real, imag) in ((0.0, here), (8.0, there)):
            hits = [position == geom[15:16] + (tap - shift) for tap in range(4)]
            cos_t = pick(hits, [jnp.broadcast_to(geom[i : i + 1], (8, cap)) for i in range(4)])
            sin_t = pick(hits, [jnp.broadcast_to(geom[4 + i : 5 + i], (8, cap)) for i in range(4)])
            first = first + cos_t * real - sin_t * imag
            second = second + cos_t * imag + sin_t * real
        return jnp.sum(first, axis=0, keepdims=True), jnp.sum(second, axis=0, keepdims=True)

    spare = chunks.shape[1] - 1

    def start_blend(which, tile, chunk):
        cols, blend = sets[which]
        build_cols(geom_ref[tile, chunk], cols.at[0], cols.at[1])
        left = jnp.concatenate([whi[...], wlo[...], whi[...]], axis=1)
        right = jnp.concatenate([cols[0], cols[0], cols[1]], axis=0)
        blend[...] = dot_f32(left, right, ((1,), (0,)))

    def finish(which, tile, chunk):
        first, second = gathered(geom_ref[tile, chunk], sets[which][1])
        chunks[tile, chunk, 0:1, :] = first
        chunks[tile, chunk, 1:2, :] = second

    def per_tile(tile, last):
        lane = lax.broadcasted_iota(jnp.int32, (fold2, TC), 1)
        after = lax.rem(tile + 1, tiles)
        before = lax.rem(tile + tiles - 1, tiles)
        rim = jnp.where(lane < TC // 2, work[after], work[before])
        high, low = halves(jnp.concatenate([work[tile], rim], axis=1))
        whi[...] = high
        wlo[...] = low

        def per_pair(pair, last):
            start_blend(0, tile, 2 * pair)
            finish(1, *last)
            start_blend(1, tile, 2 * pair + 1)
            finish(0, tile, 2 * pair)
            return tile, 2 * pair + 1

        last = lax.fori_loop(0, used[tile] // 2, per_pair, last)
        odd = lax.rem(used[tile], 2) == 1

        @pl.when(odd)
        def _():
            start_blend(0, tile, used[tile] - 1)
            finish(1, *last)
            finish(0, tile, used[tile] - 1)

        return jnp.where(odd, 0, last[0]), jnp.where(odd, spare, last[1])

    finish(1, *lax.fori_loop(0, tiles, per_tile, (0, spare)))
    fetch_all(chunks, offsets, out_ref, tiles, slabs)


def call_kernel(kernel, shape, scratch, scalars, args):
    vmem = pl.BlockSpec(memory_space=pltpu.VMEM)
    smem = pl.BlockSpec(memory_space=pltpu.SMEM)
    return pl.pallas_call(
        kernel,
        out_shape=jax.ShapeDtypeStruct(shape, jnp.float32),
        in_specs=[smem] * len(scalars) + [vmem] * len(args),
        out_specs=vmem,
        scratch_shapes=scratch,
        compiler_params=pltpu.CompilerParams(vmem_limit_bytes=VMEM_BYTES),
        cost_estimate=pl.CostEstimate(flops=4 * 10**9, bytes_accessed=10**7, transcendentals=0),
    )(*scalars, *args)


def shared(value):
    count = lax.axis_size("slab")
    copies = jnp.broadcast_to(value[None], (count,) + value.shape)
    return lax.all_to_all(copies, "slab", 0, 0, tiled=True)


def spectrum_slab(spectrum, fold):
    slabs = G // fold
    pieces = spectrum.reshape(fold // 2, 2, slabs, -1).transpose(2, 3, 1, 0) * (1.0 / (G * G))
    pieces = pieces.reshape(slabs, -1, fold)
    return lax.all_to_all(pieces, "slab", 0, 0, tiled=True)


def spectrum_rows(mine, tiles, fold):
    count = lax.axis_size("rhs")
    copies = jnp.broadcast_to(mine[None], (count,) + mine.shape)
    every = lax.all_to_all(copies, "rhs", 0, 0, tiled=True)
    columns = every.transpose(1, 0, 2, 3).reshape(G // tiles, tiles, fold)
    return columns.transpose(1, 0, 2)


def per_device(targets, counts, cell_rows, cell_cols, fractions, spectrum, noise_var):
    tiles, cap = cell_rows.shape
    slabs = lax.axis_size("slab")
    fold = G // slabs
    slot_index = lax.broadcasted_iota(jnp.int32, (tiles, cap), 1)
    live = (slot_index < counts[:, None]).astype(jnp.float32)[:, None, :]
    noise = noise_var[0]
    start = live * targets.transpose(1, 0, 2)

    own = lax.axis_index("slab").astype(jnp.int32).reshape(1)
    rows = jnp.where(live > 0, (own[0] * fold + cell_rows).astype(jnp.float32)[:, None], -1.0)
    payload = jnp.concatenate(
        [rows, cell_cols.astype(jnp.float32)[:, None], fractions.transpose(1, 0, 2), start], axis=1
    )
    every = shared(payload.reshape(-1, cap)).reshape((slabs,) + payload.shape)
    every, spectrum = lax.optimization_barrier((every, spectrum))
    start_all = every[:, :, 4:6].reshape(slabs * tiles, 2, cap)
    filled = jnp.sum((every[:, :, 0] >= 0.0).astype(jnp.int32), axis=2)
    before = [jnp.zeros((tiles,), jnp.int32)]
    for slab in range(slabs):
        before.append(before[-1] + filled[slab])
    offsets = jnp.concatenate(before[:-1])
    used = (before[-1] + (cap - 1)) // cap
    depth = slabs + 2
    geom = call_kernel(
        prepare_kernel,
        (tiles, depth, GEOM_ROWS, cap),
        [pltpu.VMEM((tiles, depth, every.shape[2], cap), jnp.float32)],
        (offsets, used, own),
        (every,),
    )
    mine = spectrum_slab(spectrum, fold)
    geom, mine = lax.optimization_barrier((geom, mine))
    spec = spectrum_rows(mine, tiles, fold)
    row_fwd, row_inv = [jnp.asarray(m) for m in row_matrices(fold // 2)]
    col_fwd, col_inv = [jnp.asarray(m) for m in col_matrices(TC)]
    mix_cos, mix_sin = [
        jnp.asarray(np.repeat(t[:, 1:2], TC, axis=1).astype(np.float32)) for t in angle_tables(fold // 2, 2, fold)
    ]
    turn_cos, turn_sin = [jnp.asarray(t.astype(np.float32)) for t in angle_tables(tiles, TC, G)]

    def vmem(shape, dtype):
        return pltpu.VMEM(shape, dtype)

    half = jnp.bfloat16
    row_table = vmem((2, 2 * fold, cap), half)
    col_table = vmem((2, WIN, cap), half)
    point_chunks = vmem((tiles, depth, 2, cap), jnp.float32)

    def partial_product(vector):
        field = call_kernel(
            spread_kernel,
            (tiles, 2 * fold, TC),
            [point_chunks, vmem((2 * fold, WIN), jnp.float32)] + [row_table, col_table] * 2,
            (offsets, used),
            (geom, vector),
        )
        return call_kernel(
            smooth_kernel,
            (slabs * tiles, 2, cap),
            [vmem((tiles, 2 * fold, TC), jnp.float32)]
            + [vmem((2 * fold, WIN), half)] * 2
            + [col_table] * 2
            + [point_chunks]
            + [vmem((2 * fold, cap), jnp.float32)] * 2,
            (offsets, used),
            (geom, field, spec, row_fwd, row_inv, col_fwd, col_inv, turn_cos, turn_sin, mix_cos, mix_sin),
        )

    def total(value):
        return jnp.sum(value, axis=(0, 2))

    def per_rhs(scale):
        return scale[None, :, None]

    direction_all = start_all
    residual_all = start_all
    direction = start
    residual = start
    solution = jnp.zeros_like(start)
    norm_now = total(start_all * start_all)
    for repeat in range(ITERS):
        partial = partial_product(direction_all)
        blocks = partial.reshape(slabs, tiles, 2, cap)
        if repeat + 1 < ITERS:
            smoothed = jnp.sum(lax.all_to_all(blocks, "slab", 0, 0, tiled=True), axis=0)
            image = live * smoothed + noise * direction
            image_all = shared(image).reshape(slabs * tiles, 2, cap)
            alpha = norm_now / total(direction_all * image_all)
            residual_all = residual_all - per_rhs(alpha) * image_all
            norm_next = total(residual_all * residual_all)
            beta = norm_next / norm_now
            solution = solution + per_rhs(alpha) * direction
            residual = residual - per_rhs(alpha) * image
            direction = residual + per_rhs(beta) * direction
            direction_all = residual_all + per_rhs(beta) * direction_all
            norm_now = norm_next
        else:
            share = total(direction_all * partial)
            extra = jnp.broadcast_to(share[None, None, :, None], (slabs, 1, 2, cap))
            blocks = jnp.concatenate([blocks, extra], axis=1)
            summed = jnp.sum(lax.all_to_all(blocks, "slab", 0, 0, tiled=True), axis=0)
            image = live * summed[:tiles] + noise * direction
            product = summed[tiles, :, 0] + noise * total(direction_all * direction_all)
            alpha = norm_now / product
            solution = solution + per_rhs(alpha) * direction
            residual = residual - per_rhs(alpha) * image
    return solution.transpose(1, 0, 2), residual.transpose(1, 0, 2)


def solution(mesh):
    placed = (
        P("rhs", "slab", None),
        P("slab"),
        P("slab", None),
        P("slab", None),
        P(None, "slab", None),
        P(None, ("slab", "rhs")),
        P(),
    )
    return jax.shard_map(
        per_device,
        mesh=mesh,
        in_specs=placed,
        out_specs=(P("rhs", "slab", None), P("rhs", "slab", None)),
        check_vma=False,
    )
```

```python
import math

import jax
import jax.numpy as jnp
import ml_dtypes
import numpy as np
from jax import lax
from jax.experimental import pallas as pl
from jax.experimental.pallas import tpu as pltpu
from jax.sharding import PartitionSpec as P

G = 2048
TC = 128
ITERS = 2
WIN = 2 * TC
GEOM_ROWS = 24
VMEM_SPARE = 2 * 1024 * 1024


def cubic_weights(fraction):
    return (
        ((-0.5 * fraction + 1.0) * fraction - 0.5) * fraction,
        (1.5 * fraction - 2.5) * fraction * fraction + 1.0,
        ((-1.5 * fraction + 2.0) * fraction + 0.5) * fraction,
        (0.5 * fraction - 0.5) * fraction * fraction,
    )


def halves_np(table):
    high = table.astype(np.float32).astype(ml_dtypes.bfloat16)
    low = (table - high.astype(np.float64)).astype(np.float32).astype(ml_dtypes.bfloat16)
    return high, low


def angle_tables(rows, cols, length):
    index = (np.arange(rows)[:, None] * np.arange(cols)[None, :]) % length
    angle = index * (2.0 * math.pi / length)
    return np.cos(angle), np.sin(angle)


def row_matrices(size):
    cos_t, sin_t = angle_tables(size, size, size)
    out = []
    for sign in (1.0, -1.0):
        high, low = halves_np(np.block([[cos_t, sign * sin_t], [-sign * sin_t, cos_t]]))
        out.append(np.concatenate([high, high, low], axis=1))
    return out


def col_matrices(size):
    cos_t, sin_t = angle_tables(size, size, size)
    out = []
    for sign in (1.0, -1.0):
        high, low = halves_np(np.block([[cos_t, -sign * sin_t], [sign * sin_t, cos_t]]))
        out.append(np.concatenate([high, high, low], axis=0))
    return out


def halves(value):
    high = value.astype(jnp.bfloat16)
    low = (value - high.astype(jnp.float32)).astype(jnp.bfloat16)
    return high, low


def fft_list(real, imag, sign):
    count = len(real)
    if count == 1:
        return real, imag
    even_r, even_i = fft_list(real[0::2], imag[0::2], sign)
    odd_r, odd_i = fft_list(real[1::2], imag[1::2], sign)
    half = count // 2
    out_r, out_i = [None] * count, [None] * count
    for k in range(half):
        cos_k = math.cos(2.0 * math.pi * k / count)
        sin_k = sign * math.sin(2.0 * math.pi * k / count)
        if k == 0:
            turn_r, turn_i = odd_r[k], odd_i[k]
        elif 4 * k == count:
            turn_r, turn_i = -sign * odd_i[k], sign * odd_r[k]
        else:
            turn_r = odd_r[k] * cos_k - odd_i[k] * sin_k
            turn_i = odd_r[k] * sin_k + odd_i[k] * cos_k
        out_r[k], out_i[k] = even_r[k] + turn_r, even_i[k] + turn_i
        out_r[k + half], out_i[k + half] = even_r[k] - turn_r, even_i[k] - turn_i
    return out_r, out_i


def dot_f32(left, right, dims):
    return lax.dot_general(left, right, (dims, ((), ())), preferred_element_type=jnp.float32)


def wide(row):
    return jnp.broadcast_to(row, (16, row.shape[1])).astype(jnp.bfloat16)


def pick(hits, values):
    out = jnp.zeros(values[0].shape, values[0].dtype)
    for hit, value in zip(hits, values):
        out = jnp.where(hit, value, out)
    return out


def patterns(inner, value_rows):
    position = lax.broadcasted_iota(jnp.int32, (16, inner.shape[1]), 0).astype(jnp.float32)
    here = [position.astype(jnp.bfloat16) == wide(inner + float(tap)) for tap in range(4)]
    there = [position.astype(jnp.bfloat16) == wide(inner + float(tap - 16)) for tap in range(4)]
    return [(pick(here, values), pick(there, values)) for values in value_rows]


def split_rows(part):
    high = part.astype(jnp.bfloat16).astype(jnp.float32)
    low = part - high
    return [[wide(half[i : i + 1]) for i in range(4)] for half in (high, low)]


def fill(block_row, groups, count, parts, stores):
    block = wide(block_row)
    for group, use_here, use_there in groups:
        here = block == jnp.bfloat16(group)
        there = block == jnp.bfloat16((group - 1) % count)
        for (part_here, part_there), store in zip(parts, stores):
            value = jnp.where(there, part_there, 0.0) if use_there else 0.0
            value = jnp.where(here, part_here, value) if use_here else value
            store(group, value.astype(jnp.bfloat16))


def store_in(table, top):
    def store(group, value):
        table[pl.ds(top + 16 * group, 16), :] = value

    return store


def build_cols(geom, table_hi, table_lo):
    inside = TC // 16
    count = WIN // 16
    groups = [(group, True, True) for group in range(inside)]
    groups += [(inside, False, True), (count - 1, True, False)]
    parts = patterns(geom[17:18], split_rows(geom[8:12]))
    fill(geom[16:17], groups, count, parts, (store_in(table_hi, 0), store_in(table_lo, 0)))


def build_rows(geom, vector, fold, table_hi, table_lo):
    first, second = vector[0:1], vector[1:2]
    real = first * geom[0:4] + second * geom[4:8]
    imag = second * geom[0:4] - first * geom[4:8]
    count = fold // 16
    parts = patterns(geom[13:14], split_rows(real) + split_rows(imag))
    stores = [store_in(table, top) for top in (0, fold) for table in (table_hi, table_lo)]
    fill(geom[12:13], [(group, True, True) for group in range(count)], count, parts, stores)


def place_all(chunks, offsets, block_at, tiles, slabs):
    cap = chunks.shape[3]
    step = math.gcd(slabs, 8)

    def some(count, carry):
        tile = count // (slabs // step)
        first = (count - tile * (slabs // step)) * step
        spots, turned = [], []
        for which in range(step):
            offset = offsets[(first + which) * tiles + tile]
            chunk = offset // cap
            shift = offset - chunk * cap
            spots.append((chunk, shift))
            turned.append(pltpu.roll(block_at(first + which, tile), shift, 1))
        lane = lax.broadcasted_iota(jnp.int32, turned[0].shape, 1)
        for (chunk, shift), block in zip(spots, turned):
            chunks[tile, chunk] = jnp.where(lane >= shift, block, chunks[tile, chunk])
            chunks[tile, chunk + 1] = jnp.where(lane < shift, block, 0.0)
        return carry

    lax.fori_loop(0, tiles * (slabs // step), some, 0)


def fetch_all(chunks, offsets, out_ref, tiles, slabs):
    cap = chunks.shape[3]
    step = math.gcd(slabs, 8)

    def some(count, carry):
        tile = count // (slabs // step)
        first = (count - tile * (slabs // step)) * step
        lane = lax.broadcasted_iota(jnp.int32, chunks.shape[2:], 1)
        turned = []
        for which in range(step):
            offset = offsets[(first + which) * tiles + tile]
            chunk = offset // cap
            shift = offset - chunk * cap
            both = jnp.where(lane >= shift, chunks[tile, chunk], chunks[tile, chunk + 1])
            turned.append(pltpu.roll(both, lax.rem(cap - shift, cap), 1))
        for which in range(step):
            out_ref[(first + which) * tiles + tile] = turned[which]
        return carry

    lax.fori_loop(0, tiles * (slabs // step), some, 0)


def circle(index):
    quarter = G // 4
    turn = (index + quarter // 2) // quarter
    x = (index - turn * quarter).astype(jnp.float32) * (2.0 * math.pi / G)
    y = x * x
    sin_x = 1.0 / 362880.0
    for term in (-1.0 / 5040.0, 1.0 / 120.0, -1.0 / 6.0, 1.0):
        sin_x = sin_x * y + term
    sin_x = sin_x * x
    cos_x = -1.0 / 3628800.0
    for term in (1.0 / 40320.0, -1.0 / 720.0, 1.0 / 24.0, -0.5, 1.0):
        cos_x = cos_x * y + term
    odd = (turn & 1) == 1
    cos_out = jnp.where(odd, sin_x, cos_x)
    sin_out = jnp.where(odd, cos_x, sin_x)
    cos_out = jnp.where(((turn + 1) & 2) == 2, -cos_out, cos_out)
    sin_out = jnp.where((turn & 2) == 2, -sin_out, sin_out)
    return cos_out, sin_out


def prepare_kernel(offsets, used, own, raw_ref, geom_ref, chunks):
    tiles, depth, _, cap = chunks.shape
    slabs = raw_ref.shape[0]
    fold = G // slabs
    chunks[...] = jnp.zeros(chunks.shape, jnp.float32)
    geom_ref[...] = jnp.zeros(geom_ref.shape, jnp.float32)
    place_all(chunks, offsets, lambda slab, tile: raw_ref[slab, tile], tiles, slabs)
    mine = own[0]
    steps = [circle((jnp.full((1, cap), tap, jnp.int32) * mine) & (G - 1)) for tap in range(1, 4)]

    def per_tile(tile, carry):
        def per_chunk(chunk, inner):
            raw = chunks[tile, chunk]
            row = jnp.maximum(raw[0:1].astype(jnp.int32), 0) + (G - 1)
            col = raw[1:2].astype(jnp.int32) + (WIN - 1)
            row_weights = cubic_weights(raw[2:3])
            col_weights = cubic_weights(raw[3:4])
            base_cos, base_sin = circle((row * mine) & (G - 1))
            for tap in range(4):
                cos_t, sin_t = base_cos, base_sin
                if tap:
                    step_cos, step_sin = steps[tap - 1]
                    cos_t = base_cos * step_cos - base_sin * step_sin
                    sin_t = base_sin * step_cos + base_cos * step_sin
                values = (row_weights[tap] * cos_t, row_weights[tap] * sin_t, col_weights[tap])
                for kind, value in enumerate(values):
                    at = 4 * kind + tap
                    geom_ref[tile, chunk, at : at + 1, :] = value
            row, col = row & (fold - 1), col & (WIN - 1)
            places = (row >> 4, row & 15, row >> 3, row & 7, col >> 4, col & 15)
            for kind, value in enumerate(places):
                at = 12 + kind
                geom_ref[tile, chunk, at : at + 1, :] = value.astype(jnp.float32)
            return inner

        lax.fori_loop(0, used[tile], per_chunk, 0)
        return carry

    lax.fori_loop(0, tiles, per_tile, 0)


def spread_kernel(offsets, used, geom_ref, vec_ref, field_ref, chunks, acc, rows0, cols0, rows1, cols1):
    tiles, fold2, _ = field_ref.shape
    slabs = vec_ref.shape[0] // tiles
    fold = fold2 // 2
    cap = chunks.shape[3]
    for table in (cols0, cols1):
        table[...] = jnp.zeros(table.shape, table.dtype)
    field_ref[...] = jnp.zeros(field_ref.shape, jnp.float32)
    chunks[...] = jnp.zeros(chunks.shape, jnp.float32)
    place_all(chunks, offsets, lambda slab, tile: vec_ref[slab * tiles + tile], tiles, slabs)
    sets = ((rows0, cols0), (rows1, cols1))

    def build(which, tile, chunk):
        rows, cols = sets[which]
        geom = geom_ref[tile, chunk]
        build_rows(geom, chunks[tile, chunk], fold, rows.at[0], rows.at[1])
        build_cols(geom, cols.at[0], cols.at[1])

    def add(which):
        rows, cols = sets[which]
        left = jnp.concatenate([rows[0], rows[1], rows[0]], axis=1)
        right = jnp.concatenate([cols[0], cols[0], cols[1]], axis=1)
        acc[...] += dot_f32(left, right, ((1,), (1,)))

    build(0, 0, 0)

    def per_tile(tile, carry):
        acc[...] = jnp.zeros(acc.shape, jnp.float32)
        behind = jnp.minimum(tile + 1, tiles - 1)

        def per_pair(pair, inner):
            more = 2 * pair + 2 < used[tile]
            add(0)
            build(1, tile, 2 * pair + 1)
            add(1)
            build(0, jnp.where(more, tile, behind), jnp.where(more, 2 * pair + 2, 0))
            return inner

        def per_four(four, inner):
            return per_pair(2 * four + 1, per_pair(2 * four, inner))

        fours = used[tile] // 4
        lax.fori_loop(0, fours, per_four, 0)

        @pl.when(used[tile] // 2 > 2 * fours)
        def _():
            per_pair(2 * fours, 0)

        @pl.when(lax.rem(used[tile], 2) == 1)
        def _():
            add(0)
            build(0, behind, 0)

        lane = lax.broadcasted_iota(jnp.int32, (fold2, TC), 1)
        rim = acc[:, TC:]
        field_ref[tile] += acc[:, :TC]
        after = lax.rem(tile + 1, tiles)
        before = lax.rem(tile + tiles - 1, tiles)
        field_ref[after] += jnp.where(lane < TC // 2, rim, 0.0)
        field_ref[before] += jnp.where(lane < TC // 2, 0.0, rim)
        return carry

    lax.fori_loop(0, tiles, per_tile, 0)


def smooth_kernel(
    offsets, used, geom_ref, field_ref, spec_ref, row_fwd, row_inv, col_fwd, col_inv,
    turn_cos, turn_sin, mix_cos, mix_sin, out_ref, work, whi, wlo, cols0, cols1, chunks, blend0, blend1,
):
    tiles, fold2, _ = field_ref.shape
    fold = fold2 // 2
    slabs = out_ref.shape[0] // tiles
    cap = geom_ref.shape[3]

    half = fold // 2
    many = math.gcd(tiles, 4)

    def product_rows(matrix, columns):
        high, low = halves(jnp.concatenate(columns, axis=1))
        result = dot_f32(matrix[...], jnp.concatenate([high, low, high], axis=0), ((1,), (0,)))
        return [result[:, TC * i : TC * (i + 1)] for i in range(len(columns))]

    def rows_forward(group, carry):
        columns = []
        for which in range(many):
            block = field_ref[many * group + which]
            real_a, real_b = block[:half], block[half:fold]
            imag_a, imag_b = block[fold : fold + half], block[fold + half :]
            real_d, imag_d = real_a - real_b, imag_a - imag_b
            columns.append(jnp.concatenate([real_a + real_b, imag_a + imag_b], axis=0))
            columns.append(
                jnp.concatenate(
                    [
                        real_d * mix_cos[...] + imag_d * mix_sin[...],
                        imag_d * mix_cos[...] - real_d * mix_sin[...],
                    ],
                    axis=0,
                )
            )
        results = product_rows(row_fwd, columns)
        for which in range(many):
            for odd in range(2):
                result = results[2 * which + odd]
                at = odd * half
                work[many * group + which, at : at + half, :] = result[:half]
                work[many * group + which, fold + at : fold + at + half, :] = result[half:]
        return carry

    def rows_inverse(group, carry):
        columns = []
        for which in range(many):
            block = work[many * group + which]
            columns.append(jnp.concatenate([block[:half], block[fold : fold + half]], axis=0))
            columns.append(jnp.concatenate([block[half:fold], block[fold + half :]], axis=0))
        results = product_rows(row_inv, columns)
        for which in range(many):
            even, odd = results[2 * which], results[2 * which + 1]
            real_t = odd[:half] * mix_cos[...] - odd[half:] * mix_sin[...]
            imag_t = odd[:half] * mix_sin[...] + odd[half:] * mix_cos[...]
            at = many * group + which
            work[at, :half, :] = even[:half] + real_t
            work[at, half:fold, :] = even[:half] - real_t
            work[at, fold : fold + half, :] = even[half:] + imag_t
            work[at, fold + half :, :] = even[half:] - imag_t
        return carry

    def tile_pass(sign):
        def step(group, carry):
            top = pl.multiple_of(8 * group, 8)
            real_at, imag_at = pl.ds(top, 8), pl.ds(fold + top, 8)
            real = [work[t, real_at, :] for t in range(tiles)]
            imag = [work[t, imag_at, :] for t in range(tiles)]

            def turned(real, imag):
                out_r, out_i = [], []
                for t in range(tiles):
                    cos_t, sin_t = turn_cos[t : t + 1, :], sign * turn_sin[t : t + 1, :]
                    out_r.append(real[t] * cos_t - imag[t] * sin_t)
                    out_i.append(real[t] * sin_t + imag[t] * cos_t)
                return out_r, out_i

            if sign < 0:
                real, imag = turned(*fft_list(real, imag, sign))
            else:
                real, imag = fft_list(*turned(real, imag), sign)
            for t in range(tiles):
                work[t, real_at, :] = real[t]
                work[t, imag_at, :] = imag[t]
            return carry

        lax.fori_loop(0, fold // 8, step, 0)

    def lane_pass():
        def product(left, matrix):
            high, low = halves(left)
            return dot_f32(jnp.concatenate([high, low, high], axis=1), matrix[...], ((1,), (0,)))

        def step(group, carry):
            ats = [many * group + which for which in range(many)]
            left = jnp.concatenate(
                [jnp.concatenate([work[at, :fold, :], work[at, fold:, :]], axis=1) for at in ats], axis=0
            )
            middle = product(left, col_fwd)
            spec = jnp.concatenate([spec_ref[at].T for at in ats], axis=0)
            middle = middle * jnp.concatenate([spec, spec], axis=1)
            result = product(middle, col_inv)
            for which, at in enumerate(ats):
                part = result[fold * which : fold * (which + 1)]
                work[at, :fold, :] = part[:, :TC]
                work[at, fold:, :] = part[:, TC:]
            return carry

        lax.fori_loop(0, tiles // many, step, 0)

    lax.fori_loop(0, tiles // many, rows_forward, 0)
    tile_pass(-1.0)
    lane_pass()
    tile_pass(1.0)
    lax.fori_loop(0, tiles // many, rows_inverse, 0)

    sets = ((cols0, blend0), (cols1, blend1))
    blend1[...] = jnp.zeros(blend1.shape, jnp.float32)
    for table in (cols0, cols1):
        table[...] = jnp.zeros(table.shape, table.dtype)
    chunks[...] = jnp.zeros(chunks.shape, jnp.float32)

    def gathered(geom, blend):
        block = jnp.broadcast_to(geom[14:15], (8, cap))
        count = fold // 8
        zero = jnp.zeros((8, cap), jnp.float32)
        here = [zero, zero]
        there = [zero, zero]
        for group in range(count):
            hit = block == float(group)
            for part in range(2):
                top = part * fold + 8 * group
                after = part * fold + 8 * ((group + 1) % count)
                here[part] = jnp.where(hit, blend[top : top + 8, :], here[part])
                there[part] = jnp.where(hit, blend[after : after + 8, :], there[part])
        position = lax.broadcasted_iota(jnp.int32, (8, cap), 0).astype(jnp.float32)
        first, second = zero, zero
        for shift, (real, imag) in ((0.0, here), (8.0, there)):
            hits = [position == geom[15:16] + (tap - shift) for tap in range(4)]
            cos_t = pick(hits, [jnp.broadcast_to(geom[i : i + 1], (8, cap)) for i in range(4)])
            sin_t = pick(hits, [jnp.broadcast_to(geom[4 + i : 5 + i], (8, cap)) for i in range(4)])
            first = first + cos_t * real - sin_t * imag
            second = second + cos_t * imag + sin_t * real
        return jnp.sum(first, axis=0, keepdims=True), jnp.sum(second, axis=0, keepdims=True)

    spare = chunks.shape[1] - 1

    def start_blend(which, tile, chunk):
        cols, blend = sets[which]
        build_cols(geom_ref[tile, chunk], cols.at[0], cols.at[1])
        left = jnp.concatenate([whi[...], wlo[...], whi[...]], axis=1)
        right = jnp.concatenate([cols[0], cols[0], cols[1]], axis=0)
        blend[...] = dot_f32(left, right, ((1,), (0,)))

    def finish(which, tile, chunk):
        first, second = gathered(geom_ref[tile, chunk], sets[which][1])
        chunks[tile, chunk, 0:1, :] = first
        chunks[tile, chunk, 1:2, :] = second

    def per_tile(tile, last):
        lane = lax.broadcasted_iota(jnp.int32, (fold2, TC), 1)
        after = lax.rem(tile + 1, tiles)
        before = lax.rem(tile + tiles - 1, tiles)
        rim = jnp.where(lane < TC // 2, work[after], work[before])
        high, low = halves(jnp.concatenate([work[tile], rim], axis=1))
        whi[...] = high
        wlo[...] = low

        def per_pair(pair, last):
            start_blend(0, tile, 2 * pair)
            finish(1, *last)
            start_blend(1, tile, 2 * pair + 1)
            finish(0, tile, 2 * pair)
            return tile, 2 * pair + 1

        def per_four(four, last):
            return per_pair(2 * four + 1, per_pair(2 * four, last))

        fours = used[tile] // 4
        last = lax.fori_loop(0, fours, per_four, last)
        pair = used[tile] // 2 > 2 * fours
        before_pair = last

        @pl.when(pair)
        def _():
            per_pair(2 * fours, before_pair)

        last = (jnp.where(pair, tile, last[0]), jnp.where(pair, 4 * fours + 1, last[1]))
        odd = lax.rem(used[tile], 2) == 1

        @pl.when(odd)
        def _():
            start_blend(0, tile, used[tile] - 1)
            finish(1, *last)
            finish(0, tile, used[tile] - 1)

        return jnp.where(odd, 0, last[0]), jnp.where(odd, spare, last[1])

    finish(1, *lax.fori_loop(0, tiles, per_tile, (0, spare)))
    fetch_all(chunks, offsets, out_ref, tiles, slabs)


def call_kernel(kernel, shape, scratch, scalars, args):
    vmem = pl.BlockSpec(memory_space=pltpu.VMEM)
    smem = pl.BlockSpec(memory_space=pltpu.SMEM)
    arrays = [(a.shape, a.dtype) for a in args] + [(shape, jnp.float32)]
    arrays += [(part.shape, part.dtype) for part in scratch]
    held = sum(math.prod(dims) * jnp.dtype(kind).itemsize for dims, kind in arrays)
    return pl.pallas_call(
        kernel,
        out_shape=jax.ShapeDtypeStruct(shape, jnp.float32),
        in_specs=[smem] * len(scalars) + [vmem] * len(args),
        out_specs=vmem,
        scratch_shapes=scratch,
        compiler_params=pltpu.CompilerParams(vmem_limit_bytes=held + held // 4 + VMEM_SPARE),
        cost_estimate=pl.CostEstimate(flops=4 * 10**9, bytes_accessed=10**7, transcendentals=0),
    )(*scalars, *args)


def shared(value):
    count = lax.axis_size("slab")
    copies = jnp.broadcast_to(value[None], (count,) + value.shape)
    return lax.all_to_all(copies, "slab", 0, 0, tiled=True)


def spectrum_pieces(spectrum, fold):
    slabs = G // fold
    pieces = spectrum.reshape(fold // 2, 2, slabs, -1).transpose(2, 3, 1, 0) * (1.0 / (G * G))
    return pieces.reshape(slabs, -1, fold)


def spectrum_rows(mine, tiles, fold):
    count = lax.axis_size("rhs")
    copies = jnp.broadcast_to(mine[None], (count,) + mine.shape)
    every = lax.all_to_all(copies, "rhs", 0, 0, tiled=True)
    columns = every.transpose(1, 0, 2, 3).reshape(G // tiles, tiles, fold)
    return columns.transpose(1, 0, 2)


def per_device(targets, counts, cell_rows, cell_cols, fractions, spectrum, noise_var):
    tiles, cap = cell_rows.shape
    slabs = lax.axis_size("slab")
    fold = G // slabs
    slot_index = lax.broadcasted_iota(jnp.int32, (tiles, cap), 1)
    live = (slot_index < counts[:, None]).astype(jnp.float32)[:, None, :]
    noise = noise_var[0]
    start = live * targets.transpose(1, 0, 2)

    own = lax.axis_index("slab").astype(jnp.int32).reshape(1)
    rows = jnp.where(live > 0, (own[0] * fold + cell_rows).astype(jnp.float32)[:, None], -1.0)
    payload = jnp.concatenate(
        [rows, cell_cols.astype(jnp.float32)[:, None], fractions.transpose(1, 0, 2), start], axis=1
    )
    every = shared(payload.reshape(-1, cap)).reshape((slabs,) + payload.shape)
    every, pieces = lax.optimization_barrier((every, spectrum_pieces(spectrum, fold)))
    start_all = every[:, :, 4:6].reshape(slabs * tiles, 2, cap)
    filled = jnp.sum((every[:, :, 0] >= 0.0).astype(jnp.int32), axis=2)
    before = [jnp.zeros((tiles,), jnp.int32)]
    for slab in range(slabs):
        before.append(before[-1] + filled[slab])
    offsets = jnp.concatenate(before[:-1])
    used = (before[-1] + (cap - 1)) // cap
    depth = slabs + 2
    geom = call_kernel(
        prepare_kernel,
        (tiles, depth, GEOM_ROWS, cap),
        [pltpu.VMEM((tiles, depth, every.shape[2], cap), jnp.float32)],
        (offsets, used, own),
        (every,),
    )
    mine = lax.all_to_all(pieces, "slab", 0, 0, tiled=True)
    geom, mine = lax.optimization_barrier((geom, mine))
    spec = spectrum_rows(mine, tiles, fold)
    row_fwd, row_inv = [jnp.asarray(m) for m in row_matrices(fold // 2)]
    col_fwd, col_inv = [jnp.asarray(m) for m in col_matrices(TC)]
    mix_cos, mix_sin = [
        jnp.asarray(np.repeat(t[:, 1:2], TC, axis=1).astype(np.float32)) for t in angle_tables(fold // 2, 2, fold)
    ]
    turn_cos, turn_sin = [jnp.asarray(t.astype(np.float32)) for t in angle_tables(tiles, TC, G)]

    def vmem(shape, dtype):
        return pltpu.VMEM(shape, dtype)

    half = jnp.bfloat16
    row_table = vmem((2, 2 * fold, cap), half)
    col_table = vmem((2, WIN, cap), half)
    point_chunks = vmem((tiles, depth, 2, cap), jnp.float32)

    def partial_product(vector):
        field = call_kernel(
            spread_kernel,
            (tiles, 2 * fold, TC),
            [point_chunks, vmem((2 * fold, WIN), jnp.float32)] + [row_table, col_table] * 2,
            (offsets, used),
            (geom, vector),
        )
        return call_kernel(
            smooth_kernel,
            (slabs * tiles, 2, cap),
            [vmem((tiles, 2 * fold, TC), jnp.float32)]
            + [vmem((2 * fold, WIN), half)] * 2
            + [col_table] * 2
            + [point_chunks]
            + [vmem((2 * fold, cap), jnp.float32)] * 2,
            (offsets, used),
            (geom, field, spec, row_fwd, row_inv, col_fwd, col_inv, turn_cos, turn_sin, mix_cos, mix_sin),
        )

    def total(value):
        return jnp.sum(value, axis=(0, 2))

    def per_rhs(scale):
        return scale[None, :, None]

    direction_all = start_all
    residual_all = start_all
    direction = start
    residual = start
    solution = jnp.zeros_like(start)
    norm_now = total(start_all * start_all)
    for repeat in range(ITERS):
        partial = partial_product(direction_all)
        blocks = partial.reshape(slabs, tiles, 2, cap)
        if repeat + 1 < ITERS:
            smoothed = jnp.sum(lax.all_to_all(blocks, "slab", 0, 0, tiled=True), axis=0)
            image = live * smoothed + noise * direction
            image_all = shared(image).reshape(slabs * tiles, 2, cap)
            alpha = norm_now / total(direction_all * image_all)
            residual_all = residual_all - per_rhs(alpha) * image_all
            norm_next = total(residual_all * residual_all)
            beta = norm_next / norm_now
            solution = solution + per_rhs(alpha) * direction
            residual = residual - per_rhs(alpha) * image
            direction = residual + per_rhs(beta) * direction
            direction_all = residual_all + per_rhs(beta) * direction_all
            norm_now = norm_next
        else:
            share = total(direction_all * partial)
            extra = jnp.broadcast_to(share[None, None, :, None], (slabs, 1, 2, cap))
            blocks = jnp.concatenate([blocks, extra], axis=1)
            summed = jnp.sum(lax.all_to_all(blocks, "slab", 0, 0, tiled=True), axis=0)
            image = live * summed[:tiles] + noise * direction
            product = summed[tiles, :, 0] + noise * total(direction_all * direction_all)
            alpha = norm_now / product
            solution = solution + per_rhs(alpha) * direction
            residual = residual - per_rhs(alpha) * image
    return solution.transpose(1, 0, 2), residual.transpose(1, 0, 2)


def solution(mesh):
    placed = (
        P("rhs", "slab", None),
        P("slab"),
        P("slab", None),
        P("slab", None),
        P(None, "slab", None),
        P(None, ("slab", "rhs")),
        P(),
    )
    return jax.shard_map(
        per_device,
        mesh=mesh,
        in_specs=placed,
        out_specs=(P("rhs", "slab", None), P("rhs", "slab", None)),
        check_vma=False,
    )
```

```python
import math

import jax
import jax.numpy as jnp
import ml_dtypes
import numpy as np
from jax import lax
from jax.experimental import pallas as pl
from jax.experimental.pallas import tpu as pltpu
from jax.sharding import PartitionSpec as P

G = 2048
TC = 128
ITERS = 2
WIN = 2 * TC
GEOM_ROWS = 24
VMEM_SPARE = 2 * 1024 * 1024


def cubic_weights(fraction):
    return (
        ((-0.5 * fraction + 1.0) * fraction - 0.5) * fraction,
        (1.5 * fraction - 2.5) * fraction * fraction + 1.0,
        ((-1.5 * fraction + 2.0) * fraction + 0.5) * fraction,
        (0.5 * fraction - 0.5) * fraction * fraction,
    )


def halves_np(table):
    high = table.astype(np.float32).astype(ml_dtypes.bfloat16)
    low = (table - high.astype(np.float64)).astype(np.float32).astype(ml_dtypes.bfloat16)
    return high, low


def angle_tables(rows, cols, length):
    index = (np.arange(rows)[:, None] * np.arange(cols)[None, :]) % length
    angle = index * (2.0 * math.pi / length)
    return np.cos(angle), np.sin(angle)


def row_matrices(size):
    cos_t, sin_t = angle_tables(size, size, size)
    out = []
    for sign in (1.0, -1.0):
        high, low = halves_np(np.block([[cos_t, sign * sin_t], [-sign * sin_t, cos_t]]))
        out.append(np.concatenate([high, low], axis=1))
    return out


def col_matrices(size):
    cos_t, sin_t = angle_tables(size, size, size)
    out = []
    for sign in (1.0, -1.0):
        high, low = halves_np(np.block([[cos_t, -sign * sin_t], [sign * sin_t, cos_t]]))
        out.append(np.concatenate([high, low], axis=0))
    return out


def halves(value):
    high = value.astype(jnp.bfloat16)
    low = (value - high.astype(jnp.float32)).astype(jnp.bfloat16)
    return high, low


def fft_list(real, imag, sign):
    count = len(real)
    if count == 1:
        return real, imag
    even_r, even_i = fft_list(real[0::2], imag[0::2], sign)
    odd_r, odd_i = fft_list(real[1::2], imag[1::2], sign)
    half = count // 2
    out_r, out_i = [None] * count, [None] * count
    for k in range(half):
        cos_k = math.cos(2.0 * math.pi * k / count)
        sin_k = sign * math.sin(2.0 * math.pi * k / count)
        if k == 0:
            turn_r, turn_i = odd_r[k], odd_i[k]
        elif 4 * k == count:
            turn_r, turn_i = -sign * odd_i[k], sign * odd_r[k]
        else:
            turn_r = odd_r[k] * cos_k - odd_i[k] * sin_k
            turn_i = odd_r[k] * sin_k + odd_i[k] * cos_k
        out_r[k], out_i[k] = even_r[k] + turn_r, even_i[k] + turn_i
        out_r[k + half], out_i[k + half] = even_r[k] - turn_r, even_i[k] - turn_i
    return out_r, out_i


def dot_f32(left, right, dims):
    return lax.dot_general(left, right, (dims, ((), ())), preferred_element_type=jnp.float32)


def wide(row):
    return jnp.broadcast_to(row, (16, row.shape[1])).astype(jnp.bfloat16)


def pick(hits, values):
    out = jnp.zeros(values[0].shape, values[0].dtype)
    for hit, value in zip(hits, values):
        out = jnp.where(hit, value, out)
    return out


def patterns(inner, value_rows):
    position = lax.broadcasted_iota(jnp.int32, (16, inner.shape[1]), 0).astype(jnp.float32)
    here = [position.astype(jnp.bfloat16) == wide(inner + float(tap)) for tap in range(4)]
    there = [position.astype(jnp.bfloat16) == wide(inner + float(tap - 16)) for tap in range(4)]
    return [(pick(here, values), pick(there, values)) for values in value_rows]


def split_rows(part):
    high = part.astype(jnp.bfloat16).astype(jnp.float32)
    low = part - high
    return [[wide(half[i : i + 1]) for i in range(4)] for half in (high, low)]


def fill(block_row, groups, count, parts, stores):
    block = wide(block_row)
    for group, use_here, use_there in groups:
        here = block == jnp.bfloat16(group)
        there = block == jnp.bfloat16((group - 1) % count)
        for (part_here, part_there), store in zip(parts, stores):
            value = jnp.where(there, part_there, 0.0) if use_there else 0.0
            value = jnp.where(here, part_here, value) if use_here else value
            store(group, value.astype(jnp.bfloat16))


def store_in(table, top):
    def store(group, value):
        table[pl.ds(top + 16 * group, 16), :] = value

    return store


def build_cols(geom, table_hi, table_lo):
    inside = TC // 16
    count = WIN // 16
    groups = [(group, True, True) for group in range(inside)]
    groups += [(inside, False, True), (count - 1, True, False)]
    parts = patterns(geom[17:18], split_rows(geom[8:12]))
    fill(geom[16:17], groups, count, parts, (store_in(table_hi, 0), store_in(table_lo, 0)))


def build_rows(geom, vector, fold, table_hi, table_lo):
    first, second = vector[0:1], vector[1:2]
    real = first * geom[0:4] + second * geom[4:8]
    imag = second * geom[0:4] - first * geom[4:8]
    count = fold // 16
    parts = patterns(geom[13:14], split_rows(real) + split_rows(imag))
    stores = [store_in(table, top) for top in (0, fold) for table in (table_hi, table_lo)]
    fill(geom[12:13], [(group, True, True) for group in range(count)], count, parts, stores)


def place_all(chunks, offsets, block_at, tiles, slabs):
    cap = chunks.shape[3]
    step = math.gcd(slabs, 8)

    def some(count, carry):
        tile = count // (slabs // step)
        first = (count - tile * (slabs // step)) * step
        spots, turned = [], []
        for which in range(step):
            offset = offsets[(first + which) * tiles + tile]
            chunk = offset // cap
            shift = offset - chunk * cap
            spots.append((chunk, shift))
            turned.append(pltpu.roll(block_at(first + which, tile), shift, 1))
        lane = lax.broadcasted_iota(jnp.int32, turned[0].shape, 1)
        for (chunk, shift), block in zip(spots, turned):
            chunks[tile, chunk] = jnp.where(lane >= shift, block, chunks[tile, chunk])
            chunks[tile, chunk + 1] = jnp.where(lane < shift, block, 0.0)
        return carry

    lax.fori_loop(0, tiles * (slabs // step), some, 0)


def fetch_all(chunks, offsets, out_ref, tiles, slabs):
    cap = chunks.shape[3]
    step = math.gcd(slabs, 8)

    def some(count, carry):
        tile = count // (slabs // step)
        first = (count - tile * (slabs // step)) * step
        lane = lax.broadcasted_iota(jnp.int32, chunks.shape[2:], 1)
        turned = []
        for which in range(step):
            offset = offsets[(first + which) * tiles + tile]
            chunk = offset // cap
            shift = offset - chunk * cap
            both = jnp.where(lane >= shift, chunks[tile, chunk], chunks[tile, chunk + 1])
            turned.append(pltpu.roll(both, lax.rem(cap - shift, cap), 1))
        for which in range(step):
            out_ref[(first + which) * tiles + tile] = turned[which]
        return carry

    lax.fori_loop(0, tiles * (slabs // step), some, 0)


def circle(index):
    quarter = G // 4
    turn = (index + quarter // 2) // quarter
    x = (index - turn * quarter).astype(jnp.float32) * (2.0 * math.pi / G)
    y = x * x
    sin_x = 1.0 / 362880.0
    for term in (-1.0 / 5040.0, 1.0 / 120.0, -1.0 / 6.0, 1.0):
        sin_x = sin_x * y + term
    sin_x = sin_x * x
    cos_x = -1.0 / 3628800.0
    for term in (1.0 / 40320.0, -1.0 / 720.0, 1.0 / 24.0, -0.5, 1.0):
        cos_x = cos_x * y + term
    odd = (turn & 1) == 1
    cos_out = jnp.where(odd, sin_x, cos_x)
    sin_out = jnp.where(odd, cos_x, sin_x)
    cos_out = jnp.where(((turn + 1) & 2) == 2, -cos_out, cos_out)
    sin_out = jnp.where((turn & 2) == 2, -sin_out, sin_out)
    return cos_out, sin_out


def prepare_kernel(offsets, used, own, raw_ref, geom_ref, chunks):
    tiles, depth, _, cap = chunks.shape
    slabs = raw_ref.shape[0]
    fold = G // slabs
    chunks[...] = jnp.zeros(chunks.shape, jnp.float32)
    geom_ref[...] = jnp.zeros(geom_ref.shape, jnp.float32)
    place_all(chunks, offsets, lambda slab, tile: raw_ref[slab, tile], tiles, slabs)
    mine = own[0]
    steps = [circle((jnp.full((1, cap), tap, jnp.int32) * mine) & (G - 1)) for tap in range(1, 4)]

    def per_tile(tile, carry):
        def per_chunk(chunk, inner):
            raw = chunks[tile, chunk]
            row = jnp.maximum(raw[0:1].astype(jnp.int32), 0) + (G - 1)
            col = raw[1:2].astype(jnp.int32) + (WIN - 1)
            row_weights = cubic_weights(raw[2:3])
            col_weights = cubic_weights(raw[3:4])
            base_cos, base_sin = circle((row * mine) & (G - 1))
            for tap in range(4):
                cos_t, sin_t = base_cos, base_sin
                if tap:
                    step_cos, step_sin = steps[tap - 1]
                    cos_t = base_cos * step_cos - base_sin * step_sin
                    sin_t = base_sin * step_cos + base_cos * step_sin
                values = (row_weights[tap] * cos_t, row_weights[tap] * sin_t, col_weights[tap])
                for kind, value in enumerate(values):
                    at = 4 * kind + tap
                    geom_ref[tile, chunk, at : at + 1, :] = value
            row, col = row & (fold - 1), col & (WIN - 1)
            places = (row >> 4, row & 15, row >> 3, row & 7, col >> 4, col & 15)
            for kind, value in enumerate(places):
                at = 12 + kind
                geom_ref[tile, chunk, at : at + 1, :] = value.astype(jnp.float32)
            return inner

        lax.fori_loop(0, used[tile], per_chunk, 0)
        return carry

    lax.fori_loop(0, tiles, per_tile, 0)


def spread_kernel(offsets, used, geom_ref, vec_ref, field_ref, chunks, acc, rows0, cols0, rows1, cols1):
    tiles, fold2, _ = field_ref.shape
    slabs = vec_ref.shape[0] // tiles
    fold = fold2 // 2
    cap = chunks.shape[3]
    for table in (cols0, cols1):
        table[...] = jnp.zeros(table.shape, table.dtype)
    field_ref[...] = jnp.zeros(field_ref.shape, jnp.float32)
    chunks[...] = jnp.zeros(chunks.shape, jnp.float32)
    place_all(chunks, offsets, lambda slab, tile: vec_ref[slab * tiles + tile], tiles, slabs)
    sets = ((rows0, cols0), (rows1, cols1))

    def build(which, tile, chunk):
        rows, cols = sets[which]
        geom = geom_ref[tile, chunk]
        build_rows(geom, chunks[tile, chunk], fold, rows.at[0], rows.at[1])
        build_cols(geom, cols.at[0], cols.at[1])

    def add(which):
        rows, cols = sets[which]
        left = jnp.concatenate([rows[0], rows[1], rows[0]], axis=1)
        right = jnp.concatenate([cols[0], cols[0], cols[1]], axis=1)
        acc[...] += dot_f32(left, right, ((1,), (1,)))

    build(0, 0, 0)

    def per_tile(tile, carry):
        acc[...] = jnp.zeros(acc.shape, jnp.float32)
        behind = jnp.minimum(tile + 1, tiles - 1)

        def per_pair(pair, inner):
            more = 2 * pair + 2 < used[tile]
            add(0)
            build(1, tile, 2 * pair + 1)
            add(1)
            build(0, jnp.where(more, tile, behind), jnp.where(more, 2 * pair + 2, 0))
            return inner

        def per_four(four, inner):
            return per_pair(2 * four + 1, per_pair(2 * four, inner))

        fours = used[tile] // 4
        lax.fori_loop(0, fours, per_four, 0)

        @pl.when(used[tile] // 2 > 2 * fours)
        def _():
            per_pair(2 * fours, 0)

        @pl.when(lax.rem(used[tile], 2) == 1)
        def _():
            add(0)
            build(0, behind, 0)

        lane = lax.broadcasted_iota(jnp.int32, (fold2, TC), 1)
        rim = acc[:, TC:]
        field_ref[tile] += acc[:, :TC]
        after = lax.rem(tile + 1, tiles)
        before = lax.rem(tile + tiles - 1, tiles)
        field_ref[after] += jnp.where(lane < TC // 2, rim, 0.0)
        field_ref[before] += jnp.where(lane < TC // 2, 0.0, rim)
        return carry

    lax.fori_loop(0, tiles, per_tile, 0)


def smooth_kernel(
    offsets, used, geom_ref, field_ref, spec_ref, row_fwd, row_inv, col_fwd, col_inv,
    turn_cos, turn_sin, mix_cos, mix_sin, out_ref, work, whi, wlo, cols0, cols1, chunks, blend0, blend1,
):
    tiles, fold2, _ = field_ref.shape
    fold = fold2 // 2
    slabs = out_ref.shape[0] // tiles
    cap = geom_ref.shape[3]

    half = fold // 2
    many = math.gcd(tiles, 4)

    def product_rows(matrix, columns):
        high, low = halves(jnp.concatenate(columns, axis=1))
        left = jnp.concatenate([matrix[:, :fold], matrix[...]], axis=1)
        result = dot_f32(left, jnp.concatenate([high, low, high], axis=0), ((1,), (0,)))
        return [result[:, TC * i : TC * (i + 1)] for i in range(len(columns))]

    def rows_forward(group, carry):
        columns = []
        for which in range(many):
            block = field_ref[many * group + which]
            real_a, real_b = block[:half], block[half:fold]
            imag_a, imag_b = block[fold : fold + half], block[fold + half :]
            real_d, imag_d = real_a - real_b, imag_a - imag_b
            columns.append(jnp.concatenate([real_a + real_b, imag_a + imag_b], axis=0))
            columns.append(
                jnp.concatenate(
                    [
                        real_d * mix_cos[...] + imag_d * mix_sin[...],
                        imag_d * mix_cos[...] - real_d * mix_sin[...],
                    ],
                    axis=0,
                )
            )
        results = product_rows(row_fwd, columns)
        for which in range(many):
            for odd in range(2):
                result = results[2 * which + odd]
                at = odd * half
                work[many * group + which, at : at + half, :] = result[:half]
                work[many * group + which, fold + at : fold + at + half, :] = result[half:]
        return carry

    def rows_inverse(group, carry):
        columns = []
        for which in range(many):
            block = work[many * group + which]
            columns.append(jnp.concatenate([block[:half], block[fold : fold + half]], axis=0))
            columns.append(jnp.concatenate([block[half:fold], block[fold + half :]], axis=0))
        results = product_rows(row_inv, columns)
        for which in range(many):
            even, odd = results[2 * which], results[2 * which + 1]
            real_t = odd[:half] * mix_cos[...] - odd[half:] * mix_sin[...]
            imag_t = odd[:half] * mix_sin[...] + odd[half:] * mix_cos[...]
            at = many * group + which
            work[at, :half, :] = even[:half] + real_t
            work[at, half:fold, :] = even[:half] - real_t
            work[at, fold : fold + half, :] = even[half:] + imag_t
            work[at, fold + half :, :] = even[half:] - imag_t
        return carry

    def tile_pass(sign):
        def step(group, carry):
            top = pl.multiple_of(8 * group, 8)
            real_at, imag_at = pl.ds(top, 8), pl.ds(fold + top, 8)
            real = [work[t, real_at, :] for t in range(tiles)]
            imag = [work[t, imag_at, :] for t in range(tiles)]

            def turned(real, imag):
                out_r, out_i = [], []
                for t in range(tiles):
                    cos_t, sin_t = turn_cos[t : t + 1, :], sign * turn_sin[t : t + 1, :]
                    out_r.append(real[t] * cos_t - imag[t] * sin_t)
                    out_i.append(real[t] * sin_t + imag[t] * cos_t)
                return out_r, out_i

            if sign < 0:
                real, imag = turned(*fft_list(real, imag, sign))
            else:
                real, imag = fft_list(*turned(real, imag), sign)
            for t in range(tiles):
                work[t, real_at, :] = real[t]
                work[t, imag_at, :] = imag[t]
            return carry

        lax.fori_loop(0, fold // 8, step, 0)

    def lane_pass():
        def product(left, matrix):
            high, low = halves(left)
            right = jnp.concatenate([matrix[:WIN], matrix[...]], axis=0)
            return dot_f32(jnp.concatenate([high, low, high], axis=1), right, ((1,), (0,)))

        def step(group, carry):
            ats = [many * group + which for which in range(many)]
            left = jnp.concatenate(
                [jnp.concatenate([work[at, :fold, :], work[at, fold:, :]], axis=1) for at in ats], axis=0
            )
            middle = product(left, col_fwd)
            spec = jnp.concatenate([spec_ref[at].T for at in ats], axis=0)
            middle = middle * jnp.concatenate([spec, spec], axis=1)
            result = product(middle, col_inv)
            for which, at in enumerate(ats):
                part = result[fold * which : fold * (which + 1)]
                work[at, :fold, :] = part[:, :TC]
                work[at, fold:, :] = part[:, TC:]
            return carry

        lax.fori_loop(0, tiles // many, step, 0)

    lax.fori_loop(0, tiles // many, rows_forward, 0)
    tile_pass(-1.0)
    lane_pass()
    tile_pass(1.0)
    lax.fori_loop(0, tiles // many, rows_inverse, 0)

    sets = ((cols0, blend0), (cols1, blend1))
    blend1[...] = jnp.zeros(blend1.shape, jnp.float32)
    for table in (cols0, cols1):
        table[...] = jnp.zeros(table.shape, table.dtype)
    chunks[...] = jnp.zeros(chunks.shape, jnp.float32)

    def gathered(geom, blend):
        block = jnp.broadcast_to(geom[14:15], (8, cap))
        count = fold // 8
        zero = jnp.zeros((8, cap), jnp.float32)
        here = [zero, zero]
        there = [zero, zero]
        for group in range(count):
            hit = block == float(group)
            for part in range(2):
                top = part * fold + 8 * group
                after = part * fold + 8 * ((group + 1) % count)
                here[part] = jnp.where(hit, blend[top : top + 8, :], here[part])
                there[part] = jnp.where(hit, blend[after : after + 8, :], there[part])
        position = lax.broadcasted_iota(jnp.int32, (8, cap), 0).astype(jnp.float32)
        first, second = zero, zero
        for shift, (real, imag) in ((0.0, here), (8.0, there)):
            hits = [position == geom[15:16] + (tap - shift) for tap in range(4)]
            cos_t = pick(hits, [jnp.broadcast_to(geom[i : i + 1], (8, cap)) for i in range(4)])
            sin_t = pick(hits, [jnp.broadcast_to(geom[4 + i : 5 + i], (8, cap)) for i in range(4)])
            first = first + cos_t * real - sin_t * imag
            second = second + cos_t * imag + sin_t * real
        return jnp.sum(first, axis=0, keepdims=True), jnp.sum(second, axis=0, keepdims=True)

    spare = chunks.shape[1] - 1

    def start_blend(which, tile, chunk):
        cols, blend = sets[which]
        build_cols(geom_ref[tile, chunk], cols.at[0], cols.at[1])
        left = jnp.concatenate([whi[...], wlo[...], whi[...]], axis=1)
        right = jnp.concatenate([cols[0], cols[0], cols[1]], axis=0)
        blend[...] = dot_f32(left, right, ((1,), (0,)))

    def finish(which, tile, chunk):
        first, second = gathered(geom_ref[tile, chunk], sets[which][1])
        chunks[tile, chunk, 0:1, :] = first
        chunks[tile, chunk, 1:2, :] = second

    def per_tile(tile, last):
        lane = lax.broadcasted_iota(jnp.int32, (fold2, TC), 1)
        after = lax.rem(tile + 1, tiles)
        before = lax.rem(tile + tiles - 1, tiles)
        rim = jnp.where(lane < TC // 2, work[after], work[before])
        high, low = halves(jnp.concatenate([work[tile], rim], axis=1))
        whi[...] = high
        wlo[...] = low

        def per_pair(pair, last):
            start_blend(0, tile, 2 * pair)
            finish(1, *last)
            start_blend(1, tile, 2 * pair + 1)
            finish(0, tile, 2 * pair)
            return tile, 2 * pair + 1

        def per_four(four, last):
            return per_pair(2 * four + 1, per_pair(2 * four, last))

        fours = used[tile] // 4
        last = lax.fori_loop(0, fours, per_four, last)
        pair = used[tile] // 2 > 2 * fours
        before_pair = last

        @pl.when(pair)
        def _():
            per_pair(2 * fours, before_pair)

        last = (jnp.where(pair, tile, last[0]), jnp.where(pair, 4 * fours + 1, last[1]))
        odd = lax.rem(used[tile], 2) == 1

        @pl.when(odd)
        def _():
            start_blend(0, tile, used[tile] - 1)
            finish(1, *last)
            finish(0, tile, used[tile] - 1)

        return jnp.where(odd, 0, last[0]), jnp.where(odd, spare, last[1])

    finish(1, *lax.fori_loop(0, tiles, per_tile, (0, spare)))
    fetch_all(chunks, offsets, out_ref, tiles, slabs)


def call_kernel(kernel, shape, scratch, scalars, args):
    vmem = pl.BlockSpec(memory_space=pltpu.VMEM)
    smem = pl.BlockSpec(memory_space=pltpu.SMEM)
    arrays = [(a.shape, a.dtype) for a in args] + [(shape, jnp.float32)]
    arrays += [(part.shape, part.dtype) for part in scratch]
    held = sum(math.prod(dims) * jnp.dtype(kind).itemsize for dims, kind in arrays)
    return pl.pallas_call(
        kernel,
        out_shape=jax.ShapeDtypeStruct(shape, jnp.float32),
        in_specs=[smem] * len(scalars) + [vmem] * len(args),
        out_specs=vmem,
        scratch_shapes=scratch,
        compiler_params=pltpu.CompilerParams(vmem_limit_bytes=held + held // 4 + VMEM_SPARE),
        cost_estimate=pl.CostEstimate(flops=4 * 10**9, bytes_accessed=10**7, transcendentals=0),
    )(*scalars, *args)


def shared(value):
    count = lax.axis_size("slab")
    copies = jnp.broadcast_to(value[None], (count,) + value.shape)
    return lax.all_to_all(copies, "slab", 0, 0, tiled=True)


def spectrum_pieces(spectrum, fold):
    slabs = G // fold
    pieces = spectrum.reshape(fold // 2, 2, slabs, -1).transpose(2, 3, 1, 0) * (1.0 / (G * G))
    return pieces.reshape(slabs, -1, fold)


def spectrum_rows(mine, tiles, fold):
    count = lax.axis_size("rhs")
    copies = jnp.broadcast_to(mine[None], (count,) + mine.shape)
    every = lax.all_to_all(copies, "rhs", 0, 0, tiled=True)
    columns = every.transpose(1, 0, 2, 3).reshape(G // tiles, tiles, fold)
    return columns.transpose(1, 0, 2)


def per_device(targets, counts, cell_rows, cell_cols, fractions, spectrum, noise_var):
    tiles, cap = cell_rows.shape
    slabs = lax.axis_size("slab")
    fold = G // slabs
    slot_index = lax.broadcasted_iota(jnp.int32, (tiles, cap), 1)
    live = (slot_index < counts[:, None]).astype(jnp.float32)[:, None, :]
    noise = noise_var[0]
    start = live * targets.transpose(1, 0, 2)

    own = lax.axis_index("slab").astype(jnp.int32).reshape(1)
    rows = jnp.where(live > 0, (own[0] * fold + cell_rows).astype(jnp.float32)[:, None], -1.0)
    payload = jnp.concatenate(
        [rows, cell_cols.astype(jnp.float32)[:, None], fractions.transpose(1, 0, 2), start], axis=1
    )
    every = shared(payload.reshape(-1, cap)).reshape((slabs,) + payload.shape)
    every, pieces = lax.optimization_barrier((every, spectrum_pieces(spectrum, fold)))
    start_all = every[:, :, 4:6].reshape(slabs * tiles, 2, cap)
    filled = jnp.sum((every[:, :, 0] >= 0.0).astype(jnp.int32), axis=2)
    before = [jnp.zeros((tiles,), jnp.int32)]
    for slab in range(slabs):
        before.append(before[-1] + filled[slab])
    offsets = jnp.concatenate(before[:-1])
    used = (before[-1] + (cap - 1)) // cap
    depth = slabs + 2
    geom = call_kernel(
        prepare_kernel,
        (tiles, depth, GEOM_ROWS, cap),
        [pltpu.VMEM((tiles, depth, every.shape[2], cap), jnp.float32)],
        (offsets, used, own),
        (every,),
    )
    mine = lax.all_to_all(pieces, "slab", 0, 0, tiled=True)
    geom, mine = lax.optimization_barrier((geom, mine))
    spec = spectrum_rows(mine, tiles, fold)
    row_fwd, row_inv = [jnp.asarray(m) for m in row_matrices(fold // 2)]
    col_fwd, col_inv = [jnp.asarray(m) for m in col_matrices(TC)]
    mix_cos, mix_sin = [
        jnp.asarray(np.repeat(t[:, 1:2], TC, axis=1).astype(np.float32)) for t in angle_tables(fold // 2, 2, fold)
    ]
    turn_cos, turn_sin = [jnp.asarray(t.astype(np.float32)) for t in angle_tables(tiles, TC, G)]

    def vmem(shape, dtype):
        return pltpu.VMEM(shape, dtype)

    half = jnp.bfloat16
    row_table = vmem((2, 2 * fold, cap), half)
    col_table = vmem((2, WIN, cap), half)
    point_chunks = vmem((tiles, depth, 2, cap), jnp.float32)

    def partial_product(vector):
        field = call_kernel(
            spread_kernel,
            (tiles, 2 * fold, TC),
            [point_chunks, vmem((2 * fold, WIN), jnp.float32)] + [row_table, col_table] * 2,
            (offsets, used),
            (geom, vector),
        )
        return call_kernel(
            smooth_kernel,
            (slabs * tiles, 2, cap),
            [vmem((tiles, 2 * fold, TC), jnp.float32)]
            + [vmem((2 * fold, WIN), half)] * 2
            + [col_table] * 2
            + [point_chunks]
            + [vmem((2 * fold, cap), jnp.float32)] * 2,
            (offsets, used),
            (geom, field, spec, row_fwd, row_inv, col_fwd, col_inv, turn_cos, turn_sin, mix_cos, mix_sin),
        )

    def total(value):
        return jnp.sum(value, axis=(0, 2))

    def per_rhs(scale):
        return scale[None, :, None]

    direction_all = start_all
    residual_all = start_all
    direction = start
    residual = start
    solution = jnp.zeros_like(start)
    norm_now = total(start_all * start_all)
    for repeat in range(ITERS):
        partial = partial_product(direction_all)
        blocks = partial.reshape(slabs, tiles, 2, cap)
        if repeat + 1 < ITERS:
            smoothed = jnp.sum(lax.all_to_all(blocks, "slab", 0, 0, tiled=True), axis=0)
            image = live * smoothed + noise * direction
            image_all = shared(image).reshape(slabs * tiles, 2, cap)
            alpha = norm_now / total(direction_all * image_all)
            residual_all = residual_all - per_rhs(alpha) * image_all
            norm_next = total(residual_all * residual_all)
            beta = norm_next / norm_now
            solution = solution + per_rhs(alpha) * direction
            residual = residual - per_rhs(alpha) * image
            direction = residual + per_rhs(beta) * direction
            direction_all = residual_all + per_rhs(beta) * direction_all
            norm_now = norm_next
        else:
            share = total(direction_all * partial)
            extra = jnp.broadcast_to(share[None, None, :, None], (slabs, 1, 2, cap))
            blocks = jnp.concatenate([blocks, extra], axis=1)
            summed = jnp.sum(lax.all_to_all(blocks, "slab", 0, 0, tiled=True), axis=0)
            image = live * summed[:tiles] + noise * direction
            product = summed[tiles, :, 0] + noise * total(direction_all * direction_all)
            alpha = norm_now / product
            solution = solution + per_rhs(alpha) * direction
            residual = residual - per_rhs(alpha) * image
    return solution.transpose(1, 0, 2), residual.transpose(1, 0, 2)


def solution(mesh):
    placed = (
        P("rhs", "slab", None),
        P("slab"),
        P("slab", None),
        P("slab", None),
        P(None, "slab", None),
        P(None, ("slab", "rhs")),
        P(),
    )
    return jax.shard_map(
        per_device,
        mesh=mesh,
        in_specs=placed,
        out_specs=(P("rhs", "slab", None), P("rhs", "slab", None)),
        check_vma=False,
    )
```
